16 devices in a mesh: data: 16 (over z, y, x, core).
Axes of the slice: x: 2, y: 2, z: 2, core: 2. Of those that a mesh axis runs over, the one named last changes fastest.
Arguments:
- w_in: float32 [2304, 384], replicated
- w_up: float32 [16, 384, 1536], replicated
- w_down: float32 [16, 1536, 384], replicated
- mom_in: float32 [2304, 384], replicated
- mom_up: float32 [16, 384, 1536], replicated
- mom_down: float32 [16, 1536, 384], replicated
- x_now: bfloat16 [8192, 2304], P('data')
- y_now: bfloat16 [8192, 384], P('data')
- x_next: bfloat16 [8192, 2304], P('data')
- y_next: bfloat16 [8192, 384], P('data')
Outputs:
- output 1: float32 [2304, 384], replicated
- output 2: float32 [16, 384, 1536], replicated
- output 3: float32 [16, 1536, 384], replicated
- output 4: float32 [2304, 384], replicated
- output 5: float32 [16, 384, 1536], replicated
- output 6: float32 [16, 1536, 384], replicated
- output 7: float32 [8192], P('data')
- output 8: float32 [8192, 384], P('data')
All inputs are finite; a program needn't handle non-finite values.
Results may differ from the reference program's by a relative error of at most 0.010136.
Values are sent between devices in bfloat16 or wider.
A program may use at most 1.25 GiB of HBM per device.

```python
import jax
import jax.numpy as jnp
from jax import lax

D = 384
FF = 1536
E = 2304
LAYERS = 16
BATCH_ROWS = 8192
STEP_SIZE = 4.0 * D / (FF * (LAYERS + 1))
MOMENTUM = 0.9


def setup_inputs(seed: int = 0) -> dict:
    key_list = jax.random.split(jax.random.key(seed), 10)
    in_scale = E ** -0.5
    up_scale = D ** -0.5
    down_scale = (FF * LAYERS) ** -0.5
    mom_factor = 0.75 / D
    return {
        "w_in": jax.random.normal(key_list[0], (E, D), jnp.float32) * in_scale,
        "w_up": jax.random.normal(key_list[1], (LAYERS, D, FF), jnp.float32) * up_scale,
        "w_down": jax.random.normal(key_list[2], (LAYERS, FF, D), jnp.float32) * down_scale,
        "mom_in": jax.random.normal(key_list[3], (E, D), jnp.float32) * (in_scale * mom_factor),
        "mom_up": jax.random.normal(key_list[4], (LAYERS, D, FF), jnp.float32) * (up_scale * mom_factor),
        "mom_down": jax.random.normal(key_list[5], (LAYERS, FF, D), jnp.float32) * (down_scale * mom_factor),
        "x_now": jax.random.normal(key_list[6], (BATCH_ROWS, E), jnp.float32).astype(jnp.bfloat16),
        "y_now": jax.random.normal(key_list[7], (BATCH_ROWS, D), jnp.float32).astype(jnp.bfloat16),
        "x_next": jax.random.normal(key_list[8], (BATCH_ROWS, E), jnp.float32).astype(jnp.bfloat16),
        "y_next": jax.random.normal(key_list[9], (BATCH_ROWS, D), jnp.float32).astype(jnp.bfloat16),
    }


def gelu_tanh(pre_value):
    return jax.nn.gelu(pre_value, approximate=True)


def stack_forward(w_in, w_up, w_down, x_rows):
    h_first = jnp.dot(x_rows, w_in.astype(jnp.bfloat16), preferred_element_type=jnp.float32)

    def layer_step(h_state, layer_weights):
        up_mat, down_mat = layer_weights
        h_low = h_state.astype(jnp.bfloat16)
        pre_act = jnp.dot(h_low, up_mat.astype(jnp.bfloat16), preferred_element_type=jnp.float32)
        act_low = gelu_tanh(pre_act).astype(jnp.bfloat16)
        h_state = h_state + jnp.dot(act_low, down_mat.astype(jnp.bfloat16), preferred_element_type=jnp.float32)
        return h_state, h_low

    return lax.scan(layer_step, h_first, (w_up, w_down))


def stack_gradients(w_in, w_up, w_down, x_rows, y_rows):
    h_last, layer_inputs = stack_forward(w_in, w_up, w_down, x_rows)
    cot_last = (h_last - y_rows.astype(jnp.float32)) / (BATCH_ROWS * D)

    def layer_back(cot_state, packed):
        up_mat, down_mat, h_low = packed
        up_low = up_mat.astype(jnp.bfloat16)
        down_low = down_mat.astype(jnp.bfloat16)
        pre_act = jnp.dot(h_low, up_low, preferred_element_type=jnp.float32)
        act_val, gelu_back = jax.vjp(gelu_tanh, pre_act)
        act_low = act_val.astype(jnp.bfloat16)
        cot_low = cot_state.astype(jnp.bfloat16)
        grad_down = jnp.dot(act_low.T, cot_low, preferred_element_type=jnp.float32)
        act_cot = jnp.dot(cot_low, down_low.T, preferred_element_type=jnp.float32)
        pre_cot = gelu_back(act_cot)[0].astype(jnp.bfloat16)
        grad_up = jnp.dot(h_low.T, pre_cot, preferred_element_type=jnp.float32)
        cot_state = cot_state + jnp.dot(pre_cot, up_low.T, preferred_element_type=jnp.float32)
        return cot_state, (grad_up, grad_down)

    cot_first, layer_grads = lax.scan(layer_back, cot_last, (w_up, w_down, layer_inputs), reverse=True)
    grad_in = jnp.dot(x_rows.T, cot_first.astype(jnp.bfloat16), preferred_element_type=jnp.float32)
    return grad_in, layer_grads[0], layer_grads[1]


def reference(w_in, w_up, w_down, mom_in, mom_up, mom_down, x_now, y_now, x_next, y_next):
    grad_in, grad_up, grad_down = stack_gradients(w_in, w_up, w_down, x_now, y_now)
    new_mom_in = MOMENTUM * mom_in + grad_in
    new_mom_up = MOMENTUM * mom_up + grad_up
    new_mom_down = MOMENTUM * mom_down + grad_down
    new_w_in = w_in - STEP_SIZE * new_mom_in
    new_w_up = w_up - STEP_SIZE * new_mom_up
    new_w_down = w_down - STEP_SIZE * new_mom_down
    h_next = stack_forward(new_w_in, new_w_up, new_w_down, x_next)[0]
    loss_next = jnp.sum(jnp.square(h_next - y_next.astype(jnp.float32)), axis=1) / (2 * D)
    return (new_w_in, new_w_up, new_w_down, new_mom_in, new_mom_up, new_mom_down, loss_next, h_next)
```

```python
import functools

import jax
import jax.numpy as jnp
from jax import lax
from jax.experimental import pallas as pl
from jax.experimental.pallas import tpu as pltpu
from jax.sharding import PartitionSpec as P

MOMENTUM = 0.9
BF = jnp.bfloat16
F32 = jnp.float32
MESH = pl.DeviceIdType.MESH
ANY = pl.BlockSpec(memory_space=pl.ANY)
VM = pl.BlockSpec(memory_space=pltpu.VMEM)
L, D, FF, E, ROWS = 16, 384, 1536, 2304, 512
NC = 3
GROUPS = ((0, 1), (1, 4), (5, 5), (10, 6))
KAPPA = 0.7978845608028654


def dot(a, b, ca, cb):
    return lax.dot_general(a, b, (((ca,), (cb,)), ((), ())), preferred_element_type=F32)


def gelu_parts(u):
    u2 = u * u
    t = jnp.tanh(u * (KAPPA + (KAPPA * 0.044715) * u2))
    cdf = 0.5 + 0.5 * t
    return u2, t, cdf


def gelu_low(u):
    _, _, cdf = gelu_parts(u)
    return (u * cdf).astype(BF)


def gelu_both(u):
    u2, t, cdf = gelu_parts(u)
    grad = cdf + (0.5 * u) * (1.0 - t * t) * (KAPPA + (3.0 * KAPPA * 0.044715) * u2)
    return (u * cdf).astype(BF), grad


def position():
    me = lax.axis_index("data")
    bits = [(me // (2 << d)) % 2 for d in range(3)]
    cores = me % 2
    partner = [me + (2 << d) * (1 - 2 * bits[d]) for d in range(3)]
    return cores, me + 1 - 2 * cores, bits, partner


class Unit:
    def __init__(self, grad, recv, hold, size, send, take, pos):
        self.grad, self.recv, self.hold = grad, recv, hold
        self.size, self.send, self.take = size, send, take
        self.core, self.mate, bits, partner = pos
        self.dims = [[(k + s) % 3 for s in range(3)] for k in range(NC)]
        self.bit = [[bits[d] for d in self.dims[k]] for k in range(NC)]
        self.to = [[partner[d] for d in self.dims[k]] for k in range(NC)]

    def rows(self, start, count):
        return pl.ds(pl.multiple_of(start, 16), count)

    def low(self, k, s):
        at = 0
        for step in range(s):
            at = at + self.bit[k][step] * (self.size >> (step + 1))
        return at

    def halving(self, k, s):
        if s == 0:
            return self.copy(self.grad(k, 1 - self.core, None), self.recv(0, k), self.mate, s, k)
        count = self.size >> s
        away = self.low(k, s - 1) + (1 - self.bit[k][s - 1]) * count
        return self.copy(self.grad(k, self.core, self.rows(away, count)), self.recv(s, k), self.to[k][s - 1], s, k)

    def doubling(self, k, s):
        part = self.rows(self.low(k, s) - self.low(k, 1), self.size >> s)
        return self.copy(self.hold(k, part), self.hold(k, part), self.to[k][s - 1], 7 - s, k)

    def copy(self, src, dst, dev, s, k):
        return pltpu.make_async_remote_copy(
            src_ref=src, dst_ref=dst, send_sem=self.send(s, k), recv_sem=self.take(s, k),
            device_id=(dev,), device_id_type=MESH)

    def start(self, s):
        for k in range(NC):
            (self.halving if s < 4 else self.doubling)(k, s if s < 4 else 7 - s).start()

    def wait(self, s, k):
        (self.halving if s < 4 else self.doubling)(k, s if s < 4 else 7 - s).wait()

    def reduce(self, s):
        for k in range(NC):
            self.wait(s, k)
            count = self.size >> s
            mine = self.grad(k, self.core, self.rows(self.low(k, s), count))
            total = mine[...] + self.recv(s, k)[...]
            if s < 3:
                mine[...] = total
                self.halving(k, s + 1).start()
            else:
                self.hold(k, self.rows(self.low(k, 3) - self.low(k, 1), count))[...] = total
                self.doubling(k, 3).start()

    def spread(self):
        for k in range(NC):
            self.wait(4, k)
            self.doubling(k, 2).start()


def first_kernel(scale, *refs):
    w_in, w_up, w_down, x_hbm, y_hbm = refs[:5]
    n_out = NC * len(GROUPS) + NC
    out = refs[5:5 + n_out]
    keep_up, keep_down = refs[5 + n_out:7 + n_out]
    (st1, st2, wb1, wb2, acts, grads, gin, r0, r1, r2, r3, q0, q1, q2, q3, hold, hin,
     xb, yb, state, low, send, take, send_in, take_in, ld1, ld2, ldx, sv1, sv2, gb1, gb2, ho, hio) = refs[7 + n_out:]
    pos = position()

    barrier = pltpu.get_barrier_semaphore()
    for dev in [pos[1]] + pos[3]:
        pl.semaphore_signal(barrier, inc=1, device_id=(dev,), device_id_type=MESH)
    pl.semaphore_wait(barrier, 4)

    def load1(l):
        return pltpu.make_async_copy(w_up.at[l], st1.at[l % 2], ld1.at[l % 2])

    def load2(l):
        return pltpu.make_async_copy(w_down.at[l], st2.at[l % 2], ld2.at[l % 2])

    def save(l):
        return (pltpu.make_async_copy(wb1.at[l % 2], keep_up.at[l], sv1.at[l % 2]),
                pltpu.make_async_copy(wb2.at[l % 2], keep_down.at[l], sv2.at[l % 2]))

    def fetch(i):
        return (pltpu.make_async_copy(keep_up.at[L - 1 - i], wb1.at[i % 2], gb1.at[i % 2]),
                pltpu.make_async_copy(keep_down.at[L - 1 - i], wb2.at[i % 2], gb2.at[i % 2]))

    load_x = pltpu.make_async_copy(x_hbm, xb, ldx.at[0])
    load_y = pltpu.make_async_copy(y_hbm, yb, ldx.at[1])
    load_a = pltpu.make_async_copy(w_in.at[pl.ds(0, 1536)], st2.at[0], ld2.at[0])
    load_b = pltpu.make_async_copy(w_in.at[pl.ds(1536, 768)], st2.at[1, pl.ds(0, 768)], ld2.at[1])
    load_x.start()
    load_a.start()
    load_b.start()
    load1(0).start()
    load1(1).start()
    load_y.start()
    load_x.wait()
    load_a.wait()
    state[...] = dot(xb[:, :1536], st2[0].astype(BF), 1, 0)
    load2(0).start()
    load_b.wait()
    state[...] += dot(xb[:, 1536:], st2[1, :768].astype(BF), 1, 0)
    load2(1).start()

    @pl.loop(0, L)
    def _(l):
        slot = l % 2
        p = state[...].astype(BF)
        acts[l] = p
        load1(l).wait()
        load2(l).wait()

        @pl.when(l >= 2)
        def _():
            for c in save(l - 2):
                c.wait()

        @pl.loop(0, 3)
        def _(j):
            total = None
            for half in range(2):
                at = pl.multiple_of(j * 512 + half * 256, 256)
                cols = pl.ds(at, 256)
                w1 = st1[slot, :, cols].astype(BF)
                wb1[slot, :, cols] = w1
                a = gelu_low(dot(p, w1, 1, 0))
                w2 = st2[slot, cols, :].astype(BF)
                wb2[slot, cols, :] = w2
                part = dot(a, w2, 1, 0)
                total = part if total is None else total + part
            state[...] += total

        for c in save(l):
            c.start()

        @pl.when(l + 2 < L)
        def _():
            load1(l + 2).start()
            load2(l + 2).start()

    for l in (L - 2, L - 1):
        for c in save(l):
            c.wait()
    for c in fetch(0):
        c.start()
    load_y.wait()
    state[...] = (state[...] - yb[...].astype(F32)) * scale

    def job(i):
        par = i % 2

        def recv(s, k):
            return (r0, r1, r2, r3)[s].at[par, k]

        def grad(k, c, rows):
            ref = grads.at[i % 4, k, c]
            return ref if rows is None else ref.at[:, rows, :]

        return Unit(grad, recv, lambda k, rows: hold.at[i % 3, k, :, rows, :], 256,
                    lambda s, k: send.at[s, par, k], lambda s, k: take.at[s, par, k], pos)

    def job_in():
        def grad(k, c, rows):
            ref = gin.at[k, c]
            return ref if rows is None else ref.at[rows, :]

        return Unit(grad, lambda s, k: (q0, q1, q2, q3)[s].at[k], lambda k, rows: hin.at[k, rows, :], 384,
                    lambda s, k: send_in.at[s, k], lambda s, k: take_in.at[s, k], pos)

    def put(i, begin):
        l = L - 1 - i
        for g, (first, count) in enumerate(GROUPS):
            @pl.when((l >= first) & (l < first + count))
            def _():
                for k in range(NC):
                    c = pltpu.make_async_copy(hold.at[i % 3, k], out[g * NC + k].at[l - first], ho.at[i % 3, k])
                    if begin:
                        c.start()
                    else:
                        c.wait()

    def middle(i):
        @pl.when((i >= 4) & (i < L + 4))
        def _():
            for k in range(NC):
                job(i - 4).wait(5, k)
            put(i - 4, True)

        @pl.when((i >= 5) & (i < L + 5))
        def _():
            put(i - 5, False)

        @pl.when((i >= 3) & (i < L + 3))
        def _():
            job(i - 3).reduce(3)

        @pl.when(i == 19)
        def _():
            job_in().reduce(3)

        @pl.when(i == 18)
        def _():
            job_in().reduce(1)

        @pl.when((i >= 2) & (i < L + 2))
        def _():
            job(i - 2).reduce(1)

        @pl.when((i >= 1) & (i < L + 1))
        def _():
            job(i - 1).reduce(0)

        @pl.when(i == 17)
        def _():
            job_in().reduce(0)

    def end(i):
        @pl.when((i >= 3) & (i < L + 3))
        def _():
            job(i - 3).spread()

        @pl.when((i >= 2) & (i < L + 2))
        def _():
            job(i - 2).reduce(2)

        @pl.when(i == 19)
        def _():
            job_in().spread()

        @pl.when(i == 18)
        def _():
            job_in().reduce(2)

        @pl.when(i < L)
        def _():
            job(i).start(0)

        @pl.when(i == 16)
        def _():
            job_in().start(0)

    @pl.loop(0, L + 4)
    def _(i):
        @pl.when(i < L)
        def _():
            @pl.when(i + 1 < L)
            def _():
                for c in fetch(i + 1):
                    c.start()

            for c in fetch(i):
                c.wait()
            low[...] = state[...].astype(BF)

        @pl.loop(0, 3)
        def _(k):
            @pl.when(k == 1)
            def _():
                middle(i)

            @pl.when(i < L)
            def _():
                slot = i % 2
                p = acts[L - 1 - i]
                cot = low[...]
                add = None
                for half in range(2):
                    at = pl.multiple_of(k * 512 + half * 256, 256)
                    cols = pl.ds(at, 256)
                    w1 = wb1[slot, :, cols]
                    w2 = wb2[slot, cols, :]
                    a, slope = gelu_both(dot(p, w1, 1, 0))
                    q = (dot(cot, w2, 1, 1) * slope).astype(BF)
                    grads[i % 4, k, half, 1] = dot(a, cot, 0, 0).astype(BF)
                    grads[i % 4, k, half, 0] = dot(q, p, 0, 0).astype(BF)
                    part = dot(q, w1, 1, 1)
                    add = part if add is None else add + part
                state[...] += add

        @pl.when(i == L)
        def _():
            low[...] = state[...].astype(BF)

            @pl.loop(0, 3)
            def _(k):
                for half in range(2):
                    cols = pl.ds(pl.multiple_of(k * 768 + half * 384, 384), 384)
                    gin[k, half] = dot(xb[:, cols], low[...], 0, 0).astype(BF)

        end(i)

    put(L - 1, False)
    for k in range(NC):
        job_in().wait(5, k)
    leave = [pltpu.make_async_copy(hin.at[k], out[NC * len(GROUPS) + k], hio.at[k]) for k in range(NC)]
    for c in leave:
        c.start()
    for c in leave:
        c.wait()


def first_call(scale, w_in, w_up, w_down, x_rows, y_rows):
    sds = jax.ShapeDtypeStruct
    shapes = [sds((count, 2, 128, D), BF) for _, count in GROUPS for _ in range(NC)]
    shapes += [sds((192, D), BF)] * NC
    shapes += [sds((L, D, FF), BF), sds((L, FF, D), BF)]
    dma = pltpu.SemaphoreType.DMA
    scratch = [
        pltpu.VMEM((2, D, FF), F32), pltpu.VMEM((2, FF, D), F32),
        pltpu.VMEM((2, D, FF), BF), pltpu.VMEM((2, FF, D), BF),
        pltpu.VMEM((L, ROWS, D), BF),
        pltpu.VMEM((4, NC, 2, 2, 256, D), BF), pltpu.VMEM((NC, 2, 384, D), BF),
        pltpu.VMEM((2, NC, 2, 256, D), BF), pltpu.VMEM((2, NC, 2, 128, D), BF),
        pltpu.VMEM((2, NC, 2, 64, D), BF), pltpu.VMEM((2, NC, 2, 32, D), BF),
        pltpu.VMEM((NC, 384, D), BF), pltpu.VMEM((NC, 192, D), BF),
        pltpu.VMEM((NC, 96, D), BF), pltpu.VMEM((NC, 48, D), BF),
        pltpu.VMEM((3, NC, 2, 128, D), BF), pltpu.VMEM((NC, 192, D), BF),
        pltpu.VMEM((ROWS, E), BF), pltpu.VMEM((ROWS, D), BF),
        pltpu.VMEM((ROWS, D), F32), pltpu.VMEM((ROWS, D), BF),
        dma((6, 2, NC)), dma((6, 2, NC)), dma((6, NC)), dma((6, NC)),
        dma((2,)), dma((2,)), dma((2,)), dma((2,)), dma((2,)), dma((2,)), dma((2,)),
        dma((3, NC)), dma((NC,)),
    ]
    res = pl.pallas_call(
        functools.partial(first_kernel, scale),
        out_shape=shapes,
        in_specs=[ANY] * 5,
        out_specs=[ANY] * len(shapes),
        scratch_shapes=scratch,
        name="train_step",
        cost_estimate=pl.CostEstimate(flops=75 * 10**9, bytes_accessed=200 * 10**6, transcendentals=0),
        compiler_params=pltpu.CompilerParams(collective_id=0, has_side_effects=True, vmem_limit_bytes=67043328),
    )(w_in, w_up, w_down, x_rows, y_rows)
    n = NC * len(GROUPS)
    return [res[g * NC:(g + 1) * NC] for g in range(len(GROUPS))], res[n:n + NC]


def entry_kernel(eta, *refs):
    parts = refs[:4 * NC]
    w_hbm, m_hbm, x_hbm = refs[4 * NC:4 * NC + 3]
    new_w, new_m, h_out = refs[4 * NC + 3:4 * NC + 6]
    wv, mv, gv, xv, gs, ins, outs = refs[4 * NC + 6:]
    core, _, bits, _ = position()
    load_g = []
    for k in range(NC):
        for n in range(4):
            c = core if n < 2 else 1 - core
            b = bits[k] if n % 2 == 0 else 1 - bits[k]
            at = pl.multiple_of(k * 768 + c * 384 + b * 192, 16)
            load_g.append(pltpu.make_async_copy(parts[k * 4 + n], gv.at[pl.ds(at, 192)], gs.at[k, n]))
    loads = [pltpu.make_async_copy(w_hbm, wv, ins.at[0]), pltpu.make_async_copy(m_hbm, mv, ins.at[1]),
             pltpu.make_async_copy(x_hbm, xv, ins.at[2])]
    for c in loads + load_g:
        c.start()
    for c in loads + load_g:
        c.wait()
    h_out[...] = jnp.zeros_like(h_out)

    @pl.loop(0, 3)
    def _(k):
        rows = pl.ds(pl.multiple_of(k * 768, 768), 768)
        m = MOMENTUM * mv[rows, :] + gv[rows, :].astype(F32)
        w = wv[rows, :] - eta * m
        mv[rows, :] = m
        wv[rows, :] = w
        pltpu.make_async_copy(wv.at[rows], new_w.at[rows], outs.at[0, k]).start()
        pltpu.make_async_copy(mv.at[rows], new_m.at[rows], outs.at[1, k]).start()
        h_out[...] += dot(xv[:, rows], w.astype(BF), 1, 0)

    @pl.loop(0, 3)
    def _(k):
        rows = pl.ds(pl.multiple_of(k * 768, 768), 768)
        pltpu.make_async_copy(wv.at[rows], new_w.at[rows], outs.at[0, k]).wait()
        pltpu.make_async_copy(mv.at[rows], new_m.at[rows], outs.at[1, k]).wait()


def entry_call(eta, parts, w_in, mom_in, x_rows):
    sds = jax.ShapeDtypeStruct
    dma = pltpu.SemaphoreType.DMA
    return pl.pallas_call(
        functools.partial(entry_kernel, eta),
        out_shape=[sds((E, D), F32), sds((E, D), F32), sds((ROWS, D), F32)],
        in_specs=[ANY] * (4 * NC + 3),
        out_specs=[ANY, ANY, VM],
        scratch_shapes=[pltpu.VMEM((E, D), F32), pltpu.VMEM((E, D), F32), pltpu.VMEM((E, D), BF),
                        pltpu.VMEM((ROWS, E), BF), dma((NC, 4)), dma((3,)), dma((2, 3))],
        name="update_in",
        cost_estimate=pl.CostEstimate(flops=5 * 10**9, bytes_accessed=20 * 10**6, transcendentals=0),
        compiler_params=pltpu.CompilerParams(vmem_limit_bytes=67043328),
    )(*[p for k in range(NC) for p in parts[k]], w_in, mom_in, x_rows)


def layers_kernel(eta, first, count, fresh, *refs):
    parts = refs[:4 * NC]
    w1_hbm, m1_hbm, w2_hbm, m2_hbm, h_in = refs[4 * NC:4 * NC + 5]
    rest = refs[4 * NC + 5 + (0 if fresh else 4):]
    new_w1, new_m1, new_w2, new_m2, h_out = rest[:5]
    v1, v2, gv, gs, ins, outs = rest[5:]
    core, _, bits, _ = position()

    def load(n):
        s = n % 3
        res = [pltpu.make_async_copy(src.at[first + n], dst.at[s, z], ins.at[s, y, z])
               for y, (a, b, dst) in enumerate(((w1_hbm, m1_hbm, v1), (w2_hbm, m2_hbm, v2)))
               for z, src in enumerate((a, b))]
        for k in range(NC):
            for r in range(4):
                c = core if r < 2 else 1 - core
                b = bits[k] if r % 2 == 0 else 1 - bits[k]
                at = pl.multiple_of(k * 512 + c * 256 + b * 128, 128)
                res.append(pltpu.make_async_copy(parts[k * 4 + r].at[n], gv.at[s, :, pl.ds(at, 128), :], gs.at[s, k, r]))
        return res

    def store(n):
        s = n % 3
        return [pltpu.make_async_copy(src.at[s, z], dst.at[first + n], outs.at[s, y, z])
                for y, (src, a, b) in enumerate(((v1, new_w1, new_m1), (v2, new_w2, new_m2)))
                for z, dst in enumerate((a, b))]

    for c in load(0):
        c.start()
    h_out[...] = h_in[...]

    @pl.loop(0, count)
    def _(n):
        s = n % 3

        @pl.when(n >= 2)
        def _():
            for c in store(n - 2):
                c.wait()

        @pl.when(n + 1 < count)
        def _():
            for c in load(n + 1):
                c.start()

        for c in load(n):
            c.wait()
        p = h_out[...].astype(BF)

        @pl.loop(0, 3)
        def _(j):
            total = None
            for half in range(2):
                cols = pl.ds(pl.multiple_of(j * 512 + half * 256, 256), 256)
                m1 = MOMENTUM * v1[s, 1, :, cols] + gv[s, 0, cols, :].astype(F32).T
                w1 = v1[s, 0, :, cols] - eta * m1
                v1[s, 1, :, cols] = m1
                v1[s, 0, :, cols] = w1
                a = gelu_low(dot(p, w1.astype(BF), 1, 0))
                m2 = MOMENTUM * v2[s, 1, cols, :] + gv[s, 1, cols, :].astype(F32)
                w2 = v2[s, 0, cols, :] - eta * m2
                v2[s, 1, cols, :] = m2
                v2[s, 0, cols, :] = w2
                part = dot(a, w2.astype(BF), 1, 0)
                total = part if total is None else total + part
            h_out[...] += total

        for c in store(n):
            c.start()

    for n in range(max(0, count - 2), count):
        for c in store(n):
            c.wait()


def layers_call(eta, first, count, parts, arrays, h, made):
    sds = jax.ShapeDtypeStruct
    dma = pltpu.SemaphoreType.DMA
    n = 4 * NC
    return pl.pallas_call(
        functools.partial(layers_kernel, eta, first, count, made is None),
        out_shape=[sds((L, D, FF), F32), sds((L, D, FF), F32), sds((L, FF, D), F32), sds((L, FF, D), F32),
                   sds((ROWS, D), F32)],
        in_specs=[ANY] * (n + 4) + [VM] + ([] if made is None else [ANY] * 4),
        out_specs=[ANY] * 4 + [VM],
        input_output_aliases={} if made is None else {n + 5 + r: r for r in range(4)},
        scratch_shapes=[pltpu.VMEM((3, 2, D, FF), F32), pltpu.VMEM((3, 2, FF, D), F32),
                        pltpu.VMEM((3, 2, FF, D), BF), dma((3, NC, 4)), dma((3, 2, 2)), dma((3, 2, 2))],
        name=f"update_{first}",
        cost_estimate=pl.CostEstimate(flops=count * 6 * 10**9, bytes_accessed=count * 21 * 10**6, transcendentals=0),
        compiler_params=pltpu.CompilerParams(vmem_limit_bytes=67043328),
    )(*[p for k in range(NC) for p in parts[k]], *arrays, h, *(made or ()))


def solution(mesh):
    group_size = mesh.shape["data"]

    def swap(v, bit):
        return lax.ppermute(v, "data", [(d, d ^ bit) for d in range(group_size)])

    def gather(own):
        res = []
        other = [swap(own[k], 2 << k) for k in range(NC)]
        for k in range(NC):
            res.append((own[k], other[k], swap(own[k], 1), swap(other[k], 1)))
        return res

    def device_steps(w_in, w_up, w_down, mom_in, mom_up, mom_down, x_now, y_now, x_next, y_next):
        eta = 4.0 * D / (FF * (L + 1))
        scale = 1.0 / (ROWS * group_size * D)
        held, held_in = first_call(scale, w_in, w_up, w_down, x_now, y_now)
        parts_in = gather(held_in)
        parts = [gather(h) for h in held]
        new_w_in, new_mom_in, h = entry_call(eta, parts_in, w_in, mom_in, x_next)
        made = None
        for (first, count), part in zip(GROUPS, parts):
            *made, h = layers_call(eta, first, count, part, (w_up, mom_up, w_down, mom_down), h, made)
        new_w_up, new_mom_up, new_w_down, new_mom_down = made
        loss = jnp.sum(jnp.square(h - y_next.astype(F32)), axis=1) / (2 * D)
        return (new_w_in, new_w_up, new_w_down, new_mom_in, new_mom_up, new_mom_down, loss, h)

    param_spec = P()
    row_spec = P("data", None)
    return jax.shard_map(
        device_steps,
        mesh=mesh,
        in_specs=(param_spec,) * 6 + (row_spec,) * 4,
        out_specs=(param_spec,) * 6 + (P("data"), row_spec),
        check_vma=False,
    )
```

```python
import functools

import jax
import jax.numpy as jnp
from jax import lax
from jax.experimental import pallas as pl
from jax.experimental.pallas import tpu as pltpu
from jax.sharding import PartitionSpec as P


MOMENTUM = 0.9
BF = jnp.bfloat16
F32 = jnp.float32
MESH = pl.DeviceIdType.MESH
ANY = pl.BlockSpec(memory_space=pl.ANY)
VM = pl.BlockSpec(memory_space=pltpu.VMEM)
L, D, FF, E, ROWS = 16, 384, 1536, 2304, 512
NC = 3
GROUPS = ((0, 1), (1, 3), (4, 5), (9, 7))
N_OUT = NC * (2 * len(GROUPS) + 6)
KAPPA = 0.7978845608028654


def dot(a, b, ca, cb):
    return lax.dot_general(a, b, (((ca,), (cb,)), ((), ())), preferred_element_type=F32)


def gelu_parts(u):
    u2 = u * u
    t = jnp.tanh(u * (KAPPA + (KAPPA * 0.044715) * u2))
    cdf = 0.5 + 0.5 * t
    return u2, t, cdf


def gelu_low(u):
    _, _, cdf = gelu_parts(u)
    return (u * cdf).astype(BF)


def gelu_both(u):
    u2, t, cdf = gelu_parts(u)
    grad = cdf + (0.5 * u) * (1.0 - t * t) * (KAPPA + (3.0 * KAPPA * 0.044715) * u2)
    return (u * cdf).astype(BF), grad


def position():
    me = lax.axis_index("data")
    bits = [(me // (2 << d)) % 2 for d in range(3)]
    cores = me % 2
    partner = [me + (2 << d) * (1 - 2 * bits[d]) for d in range(3)]
    return cores, me + 1 - 2 * cores, bits, partner


class Unit:
    def __init__(self, grad, recv, hold, whole, size, send, take, pos):
        self.grad, self.recv, self.hold, self.whole = grad, recv, hold, whole
        self.size, self.send, self.take = size, send, take
        self.core, self.mate, bits, partner = pos
        self.dims = [[(k + s) % 3 for s in range(3)] for k in range(NC)]
        self.bit = [[bits[d] for d in self.dims[k]] for k in range(NC)]
        self.to = [[partner[d] for d in self.dims[k]] for k in range(NC)]

    def rows(self, start, count):
        return pl.ds(pl.multiple_of(start, 16), count)

    def low(self, k, s):
        at = 0
        for step in range(s):
            at = at + self.bit[k][step] * (self.size >> (step + 1))
        return at

    def halving(self, k, s):
        if s == 0:
            return self.copy(self.grad(k, 1 - self.core, None), self.recv(0, k), self.mate, s, k)
        count = self.size >> s
        away = self.low(k, s - 1) + (1 - self.bit[k][s - 1]) * count
        return self.copy(self.grad(k, self.core, self.rows(away, count)), self.recv(s, k), self.to[k][s - 1], s, k)

    def doubling(self, k, s):
        part = self.rows(self.low(k, s) - self.low(k, 1), self.size >> s)
        return self.copy(self.hold(k, part), self.hold(k, part), self.to[k][s - 1], 7 - s, k)

    def across(self, k, s):
        own, mine, far, both = self.whole
        src, dst, dev = {6: (own, mine, self.mate), 7: (own, far, self.to[k][0]), 8: (far, both, self.mate)}[s]
        return self.copy(src(k), dst(k), dev, s, k)

    def step(self, s, k):
        if s < 4:
            return self.halving(k, s)
        return self.doubling(k, 7 - s) if s < 6 else self.across(k, s)

    def copy(self, src, dst, dev, s, k):
        return pltpu.make_async_remote_copy(
            src_ref=src, dst_ref=dst, send_sem=self.send(s, k), recv_sem=self.take(s, k),
            device_id=(dev,), device_id_type=MESH)

    def start(self, s):
        for k in range(NC):
            self.step(s, k).start()

    def wait(self, s):
        for k in range(NC):
            self.step(s, k).wait()

    def follow(self, s, *nexts):
        for k in range(NC):
            self.step(s, k).wait()
            for n in nexts:
                self.step(n, k).start()

    def reduce(self, s):
        for k in range(NC):
            self.step(s, k).wait()
            count = self.size >> s
            mine = self.grad(k, self.core, self.rows(self.low(k, s), count))
            total = mine[...] + self.recv(s, k)[...]
            if s < 3:
                mine[...] = total
                self.halving(k, s + 1).start()
            else:
                self.hold(k, self.rows(self.low(k, 3) - self.low(k, 1), count))[...] = total
                self.doubling(k, 3).start()


def first_kernel(scale, *refs):
    w_in, w_up, w_down, x_hbm, y_hbm = refs[:5]
    n_out = N_OUT
    out = refs[5:5 + n_out]
    (st1, st2, acts, grads, gin, r0, r1, r2, r3, q0, q1, q2, q3, hold, mates, far, both, hin, min_, fin, bin_,
     xb, yb, state, low, send, take, send_in, take_in, ld1, ld2, ldx, ho, hx) = refs[5 + n_out:]
    pos = position()

    barrier = pltpu.get_barrier_semaphore()
    for dev in [pos[1]] + pos[3]:
        pl.semaphore_signal(barrier, inc=1, device_id=(dev,), device_id_type=MESH)
    pl.semaphore_wait(barrier, 4)

    def load1(l):
        return pltpu.make_async_copy(w_up.at[l], st1.at[l % 2], ld1.at[l % 2])

    def load2(l):
        return pltpu.make_async_copy(w_down.at[l], st2.at[l % 2], ld2.at[l % 2])

    load_x = pltpu.make_async_copy(x_hbm, xb, ldx.at[0])
    load_y = pltpu.make_async_copy(y_hbm, yb, ldx.at[1])
    load_a = pltpu.make_async_copy(w_in.at[pl.ds(0, 1536)], st2.at[0], ld2.at[0])
    load_b = pltpu.make_async_copy(w_in.at[pl.ds(1536, 768)], st2.at[1, pl.ds(0, 768)], ld2.at[1])
    load_x.start()
    load_a.start()
    load_b.start()
    load1(0).start()
    load1(1).start()
    load_y.start()
    load_x.wait()
    load_a.wait()
    state[...] = dot(xb[:, :1536], st2[0].astype(BF), 1, 0)
    load2(0).start()
    load_b.wait()
    state[...] += dot(xb[:, 1536:], st2[1, :768].astype(BF), 1, 0)
    load2(1).start()

    @pl.loop(0, L)
    def _(l):
        slot = l % 2
        p = state[...].astype(BF)
        acts[l] = p
        load1(l).wait()
        load2(l).wait()

        for j in range(3):
            cols = slice(j * 512, j * 512 + 512)
            a = gelu_low(dot(p, st1[slot, :, cols].astype(BF), 1, 0))
            state[...] += dot(a, st2[slot, cols, :].astype(BF), 1, 0)

        @pl.when(l + 2 < L)
        def _():
            load1(l + 2).start()
            load2(l + 2).start()

    load_y.wait()
    state[...] = (state[...] - yb[...].astype(F32)) * scale

    def job(i):
        par = i % 2

        def recv(s, k):
            return (r0, r1, r2, r3)[s].at[par, k]

        def grad(k, c, rows):
            ref = grads.at[i % 4, k, c]
            return ref if rows is None else ref.at[:, rows, :]

        whole = (lambda k: hold.at[i % 4, k], lambda k: mates.at[i % 3, k], lambda k: far.at[k], lambda k: both.at[k])
        return Unit(grad, recv, lambda k, rows: hold.at[i % 4, k, :, rows, :], whole, 256,
                    lambda s, k: send.at[s, par, k], lambda s, k: take.at[s, par, k], pos)

    def job_in():
        def grad(k, c, rows):
            ref = gin.at[k, c]
            return ref if rows is None else ref.at[rows, :]

        return Unit(grad, lambda s, k: (q0, q1, q2, q3)[s].at[k], lambda k, rows: hin.at[k, rows, :],
                    tuple((lambda k, ref=ref: ref.at[k]) for ref in (hin, min_, fin, bin_)), 384,
                    lambda s, k: send_in.at[s, k], lambda s, k: take_in.at[s, k], pos)

    def put(i, which, begin):
        l = L - 1 - i
        for g, (first, count) in enumerate(GROUPS):
            @pl.when((l >= first) & (l < first + count))
            def _():
                for k in range(NC):
                    c = pltpu.make_async_copy(hold.at[i % 4, k] if which == 0 else mates.at[i % 3, k],
                                              out[(g * 2 + which) * NC + k].at[l - first], ho.at[i % 2, which, k])
                    if begin:
                        c.start()
                    else:
                        c.wait()

    def during(i, lag, step):
        pl.when((i >= lag) & (i < L + lag))(step)

    def middle(i):
        during(i, 2, lambda: job(i - 2).reduce(1))
        pl.when(i == 18)(lambda: job_in().reduce(1))
        during(i, 1, lambda: job(i - 1).reduce(0))
        pl.when(i == 17)(lambda: job_in().reduce(0))

        @functools.partial(during, i, 6)
        def _():
            put(i - 6, 0, False)
            put(i - 6, 1, False)

        during(i, 3, lambda: job(i - 3).reduce(3))
        pl.when(i == 19)(lambda: job_in().reduce(3))

        @functools.partial(during, i, 5)
        def _():
            job(i - 5).follow(5, 6)
            put(i - 5, 0, True)

        pl.when(i == L + 4)(lambda: job(L - 1).start(7))
        during(i, 4, lambda: job(i - 4).follow(4, 5))

    def end(i):
        during(i, 2, lambda: job(i - 2).reduce(2))
        pl.when(i == 18)(lambda: job_in().reduce(2))
        pl.when(i == 19)(lambda: job_in().follow(4, 5))

        @functools.partial(during, i, 5)
        def _():
            job(i - 5).wait(6)
            put(i - 5, 1, True)

        during(i, 0, lambda: job(i).start(0))
        pl.when(i == L)(lambda: job_in().start(0))

    @pl.loop(0, L + 5)
    def _(i):
        @pl.when(i < L)
        def _():
            @pl.when(i >= 2)
            def _():
                load1(L - 1 - i).wait()
                load2(L - 1 - i).wait()

            low[...] = state[...].astype(BF)

        @pl.loop(0, 3)
        def _(k):
            @pl.when(k == 1)
            def _():
                middle(i)

            @pl.when(i < L)
            def _():
                slot = (L - 1 - i) % 2
                p = acts[L - 1 - i]
                cot = low[...]
                add = None
                for half in range(2):
                    at = pl.multiple_of(k * 512 + half * 256, 256)
                    cols = pl.ds(at, 256)
                    w1 = st1[slot, :, cols].astype(BF)
                    w2 = st2[slot, cols, :].astype(BF)
                    a, slope = gelu_both(dot(p, w1, 1, 0))
                    q = (dot(cot, w2, 1, 1) * slope).astype(BF)
                    grads[i % 4, k, half, 1] = dot(a, cot, 0, 0).astype(BF)
                    grads[i % 4, k, half, 0] = dot(q, p, 0, 0).astype(BF)
                    part = dot(q, w1, 1, 1)
                    add = part if add is None else add + part
                state[...] += add

        @pl.when(i + 2 < L)
        def _():
            load1(L - 3 - i).start()
            load2(L - 3 - i).start()

        @pl.when(i == L)
        def _():
            low[...] = state[...].astype(BF)

            @pl.loop(0, 3)
            def _(k):
                for half in range(2):
                    cols = pl.ds(pl.multiple_of(k * 768 + half * 384, 384), 384)
                    gin[k, half] = dot(xb[:, cols], low[...], 0, 0).astype(BF)

        end(i)

    last, entry = job(L - 1), job_in()
    entry.follow(5, 7, 6)
    last.follow(7, 8)
    entry.follow(7, 8)
    entry.wait(6)
    last.wait(8)
    entry.wait(8)
    put(L - 1, 0, False)
    put(L - 1, 1, False)
    base = 2 * NC * len(GROUPS)
    leave = []
    for n, ref in enumerate((hin, min_, fin, bin_, far, both)):
        for k in range(NC):
            dst = out[base + n * NC + k]
            leave.append(pltpu.make_async_copy(ref.at[k], dst if n < 4 else dst.at[0], hx.at[n, k]))
    for c in leave:
        c.start()
    for c in leave:
        c.wait()


def first_call(scale, w_in, w_up, w_down, x_rows, y_rows):
    sds = jax.ShapeDtypeStruct
    shapes = [sds((count, 2, 128, D), BF) for _, count in GROUPS for _ in range(2 * NC)]
    shapes += [sds((192, D), BF)] * (4 * NC) + [sds((1, 2, 128, D), BF)] * (2 * NC)
    dma = pltpu.SemaphoreType.DMA
    scratch = [
        pltpu.VMEM((2, D, FF), F32), pltpu.VMEM((2, FF, D), F32),
        pltpu.VMEM((L, ROWS, D), BF),
        pltpu.VMEM((4, NC, 2, 2, 256, D), BF), pltpu.VMEM((NC, 2, 384, D), BF),
        pltpu.VMEM((2, NC, 2, 256, D), BF), pltpu.VMEM((2, NC, 2, 128, D), BF),
        pltpu.VMEM((2, NC, 2, 64, D), BF), pltpu.VMEM((2, NC, 2, 32, D), BF),
        pltpu.VMEM((NC, 384, D), BF), pltpu.VMEM((NC, 192, D), BF),
        pltpu.VMEM((NC, 96, D), BF), pltpu.VMEM((NC, 48, D), BF),
        pltpu.VMEM((4, NC, 2, 128, D), BF), pltpu.VMEM((3, NC, 2, 128, D), BF),
        pltpu.VMEM((NC, 2, 128, D), BF), pltpu.VMEM((NC, 2, 128, D), BF),
        pltpu.VMEM((NC, 192, D), BF), pltpu.VMEM((NC, 192, D), BF),
        pltpu.VMEM((NC, 192, D), BF), pltpu.VMEM((NC, 192, D), BF),
        pltpu.VMEM((ROWS, E), BF), pltpu.VMEM((ROWS, D), BF),
        pltpu.VMEM((ROWS, D), F32), pltpu.VMEM((ROWS, D), BF),
        dma((9, 2, NC)), dma((9, 2, NC)), dma((9, NC)), dma((9, NC)),
        dma((2,)), dma((2,)), dma((2,)), dma((2, 2, NC)), dma((6, NC)),
    ]
    res = pl.pallas_call(
        functools.partial(first_kernel, scale),
        out_shape=shapes,
        in_specs=[ANY] * 5,
        out_specs=[ANY] * len(shapes),
        scratch_shapes=scratch,
        name="train_step",
        cost_estimate=pl.CostEstimate(flops=75 * 10**9, bytes_accessed=200 * 10**6, transcendentals=0),
        compiler_params=pltpu.CompilerParams(collective_id=0, has_side_effects=True, vmem_limit_bytes=67043328),
    )(w_in, w_up, w_down, x_rows, y_rows)
    take3 = lambda n: res[n * NC:(n + 1) * NC]
    n = 2 * len(GROUPS)
    pairs = [(take3(2 * g), take3(2 * g + 1)) for g in range(len(GROUPS))]
    return pairs, [take3(n + r) for r in range(6)]


def layers_kernel(eta, first, count, head, *refs):
    n_parts = 4 * NC * (2 if head else 1)
    parts = refs[:4 * NC]
    w1_hbm, m1_hbm, w2_hbm, m2_hbm, h_hbm = refs[n_parts:n_parts + 5]
    rest = refs[n_parts + 5 + (2 if head else 4):]
    if head:
        parts_in = refs[4 * NC:n_parts]
        w_hbm, m_hbm = refs[n_parts + 5:n_parts + 7]
        new_win, new_min = rest[:2]
        rest = rest[2:]
    new_w1, new_m1, new_w2, new_m2, h_out = rest[:5]
    v1, v2, gv, hv, av, gs, ins, outs, hs = rest[5:14]
    core, _, bits, _ = position()

    def load(n, y):
        s = n % 3
        res = [pltpu.make_async_copy(src.at[first + n], dst.at[s, z], ins.at[s, y, z])
               for yy, (a, b, dst) in enumerate(((w1_hbm, m1_hbm, v1), (w2_hbm, m2_hbm, v2)))
               for z, src in enumerate((a, b)) if yy == y]
        for k in range(NC):
            for r in range(4):
                c = core if r < 2 else 1 - core
                b = bits[k] if r % 2 == 0 else 1 - bits[k]
                at = pl.multiple_of(k * 512 + c * 256 + b * 128, 128)
                res.append(pltpu.make_async_copy(parts[k * 4 + r].at[n, y], gv.at[s, y, pl.ds(at, 128), :],
                                                 gs.at[s, y, k, r]))
        return res

    def store(n, y):
        s = n % 3
        return [pltpu.make_async_copy(src.at[s, z], dst.at[first + n], outs.at[s, y, z])
                for yy, (src, a, b) in enumerate(((v1, new_w1, new_m1), (v2, new_w2, new_m2)))
                for z, dst in enumerate((a, b)) if yy == y]

    load_h = pltpu.make_async_copy(h_hbm, rest[14] if head else hv, hs.at[0])
    if head:
        xv, wv, mv, gi, gsi, insi, outsi = rest[14:]

        def load_in(k):
            rows = pl.ds(k * 768, 768)
            res = [pltpu.make_async_copy(w_hbm.at[rows], wv.at[rows], insi.at[0, k]),
                   pltpu.make_async_copy(m_hbm.at[rows], mv.at[rows], insi.at[1, k])]
            for r in range(4):
                c = core if r < 2 else 1 - core
                b = bits[k] if r % 2 == 0 else 1 - bits[k]
                at = pl.multiple_of(k * 768 + c * 384 + b * 192, 16)
                res.append(pltpu.make_async_copy(parts_in[k * 4 + r], gi.at[pl.ds(at, 192)], gsi.at[k, r]))
            return res

        def store_in(k):
            rows = pl.ds(k * 768, 768)
            return [pltpu.make_async_copy(wv.at[rows], new_win.at[rows], outsi.at[0, k]),
                    pltpu.make_async_copy(mv.at[rows], new_min.at[rows], outsi.at[1, k])]

        for c in load_in(0) + [load_h] + load_in(1) + load_in(2) + load(0, 0) + load(0, 1):
            c.start()
        for k in range(NC):
            for c in load_in(k) + ([load_h] if k == 0 else []):
                c.wait()
            rows = slice(k * 768, k * 768 + 768)
            m = MOMENTUM * mv[rows, :] + gi[rows, :].astype(F32)
            w = wv[rows, :] - eta * m
            mv[rows, :] = m
            wv[rows, :] = w
            for c in store_in(k):
                c.start()
            part = dot(xv[:, rows], w.astype(BF), 1, 0)
            hv[...] = part if k == 0 else hv[...] + part
    else:
        for c in load(0, 0) + [load_h] + load(0, 1):
            c.start()
        load_h.wait()

    @pl.loop(0, count)
    def _(n):
        s = n % 3

        @pl.when(n >= 2)
        def _():
            for c in store(n - 2, 0) + store(n - 2, 1):
                c.wait()

        @pl.when(n + 1 < count)
        def _():
            for c in load(n + 1, 0) + load(n + 1, 1):
                c.start()

        for c in load(n, 0):
            c.wait()
        p = hv[...].astype(BF)

        @pl.loop(0, 3)
        def _(j):
            for half in range(2):
                cols = pl.ds(pl.multiple_of(j * 512 + half * 256, 256), 256)
                m1 = MOMENTUM * v1[s, 1, :, cols] + gv[s, 0, cols, :].astype(F32).T
                w1 = v1[s, 0, :, cols] - eta * m1
                v1[s, 1, :, cols] = m1
                v1[s, 0, :, cols] = w1
                av[:, cols] = gelu_low(dot(p, w1.astype(BF), 1, 0))

        for c in store(n, 0):
            c.start()
        for c in load(n, 1):
            c.wait()

        @pl.loop(0, 3)
        def _(j):
            cols = pl.ds(pl.multiple_of(j * 512, 512), 512)
            m2 = MOMENTUM * v2[s, 1, cols, :] + gv[s, 1, cols, :].astype(F32)
            w2 = v2[s, 0, cols, :] - eta * m2
            v2[s, 1, cols, :] = m2
            v2[s, 0, cols, :] = w2
            hv[...] += dot(av[:, cols], w2.astype(BF), 1, 0)

        for c in store(n, 1):
            c.start()

    give_h = pltpu.make_async_copy(hv, h_out, hs.at[1])
    give_h.start()
    for n in range(max(0, count - 2), count):
        for c in store(n, 0) + store(n, 1):
            c.wait()
    if head:
        for k in range(NC):
            for c in store_in(k):
                c.wait()
    give_h.wait()


def layers_call(eta, first, count, parts, arrays, h, made, head=None):
    sds = jax.ShapeDtypeStruct
    dma = pltpu.SemaphoreType.DMA
    flat = [p for k in range(NC) for p in parts[k]]
    if head:
        flat += [p for k in range(NC) for p in head[0][k]]
    n = len(flat)
    more = list(head[1:]) if head else list(made)
    shapes = [sds((E, D), F32)] * 2 if head else []
    shapes += [sds((L, D, FF), F32), sds((L, D, FF), F32), sds((L, FF, D), F32), sds((L, FF, D), F32),
               sds((ROWS, D), F32)]
    scratch = [pltpu.VMEM((3, 2, D, FF), F32), pltpu.VMEM((3, 2, FF, D), F32),
               pltpu.VMEM((3, 2, FF, D), BF), pltpu.VMEM((ROWS, D), F32), pltpu.VMEM((ROWS, FF), BF),
               dma((3, 2, NC, 4)), dma((3, 2, 2)), dma((3, 2, 2)), dma((2,))]
    if head:
        scratch += [pltpu.VMEM((ROWS, E), BF), pltpu.VMEM((E, D), F32), pltpu.VMEM((E, D), F32),
                    pltpu.VMEM((E, D), BF), dma((NC, 4)), dma((2, NC)), dma((2, NC))]
    return pl.pallas_call(
        functools.partial(layers_kernel, eta, first, count, head is not None),
        out_shape=shapes,
        in_specs=[ANY] * (n + 5 + len(more)),
        out_specs=[ANY] * len(shapes),
        input_output_aliases={} if head else {n + 5 + r: r for r in range(4)},
        scratch_shapes=scratch,
        cost_estimate=pl.CostEstimate(flops=count * 6 * 10**9, bytes_accessed=count * 21 * 10**6, transcendentals=0),
        compiler_params=pltpu.CompilerParams(vmem_limit_bytes=67043328),
    )(*flat, *arrays, h, *more)


def solution(mesh):
    group_size = mesh.shape["data"]

    def swap(v, bit):
        return lax.ppermute(v, "data", [(d, d ^ bit) for d in range(group_size)])

    def far_half(own):
        res = []
        for k in range(NC):
            res.append(swap(own[k], 2 << k))
        return res

    def complete(own, mate, other, after):
        other = lax.optimization_barrier((*other, after))[:NC]
        res = []
        for k in range(NC):
            res.append((own[k], other[k], mate[k], swap(other[k], 1)))
        return res

    def device_steps(w_in, w_up, w_down, mom_in, mom_up, mom_down, x_now, y_now, x_next, y_next):
        eta = 4.0 * D / (FF * (L + 1))
        scale = 1.0 / (ROWS * group_size * D)
        pairs, (own, mate, other, both, other0, both0) = first_call(scale, w_in, w_up, w_down, x_now, y_now)
        parts_in = [(own[k], other[k], mate[k], both[k]) for k in range(NC)]
        parts = [[(pairs[0][0][k], other0[k], pairs[0][1][k], both0[k]) for k in range(NC)]]
        others = [far_half(pair[0]) for pair in pairs[1:]]
        arrays = (w_up, mom_up, w_down, mom_down)
        after = pairs[0][0][0]
        for g, (first, count) in enumerate(GROUPS):
            if g == 0:
                new_w_in, new_mom_in, *made, h = layers_call(eta, first, count, parts[0], arrays, x_next, None,
                                                             (parts_in, w_in, mom_in))
                after = h
                continue
            parts.append(complete(*pairs[g], others[g - 1], h if g == 2 else after))
            after = h
            *made, h = layers_call(eta, first, count, parts[g], arrays, h, made)
        new_w_up, new_mom_up, new_w_down, new_mom_down = made
        loss = jnp.sum(jnp.square(h - y_next.astype(F32)), axis=1) / (2 * D)
        return (new_w_in, new_w_up, new_w_down, new_mom_in, new_mom_up, new_mom_down, loss, h)

    param_spec = P()
    row_spec = P("data", None)
    return jax.shard_map(
        device_steps,
        mesh=mesh,
        in_specs=(param_spec,) * 6 + (row_spec,) * 4,
        out_specs=(param_spec,) * 6 + (P("data"), row_spec),
        check_vma=False,
    )
```

```python
import functools

import jax
import jax.numpy as jnp
from jax import lax
from jax.experimental import pallas as pl
from jax.experimental.pallas import tpu as pltpu
from jax.sharding import PartitionSpec as P


MOMENTUM = 0.9
BF = jnp.bfloat16
F32 = jnp.float32
MESH = pl.DeviceIdType.MESH
ANY = pl.BlockSpec(memory_space=pl.ANY)
VM = pl.BlockSpec(memory_space=pltpu.VMEM)
L, D, FF, E, ROWS = 16, 384, 1536, 2304, 512
NC = 3
GROUPS = ((0, 1), (1, 2), (3, 4), (7, 9))
N_OUT = NC * (2 * len(GROUPS) + 6)
KAPPA = 0.7978845608028654


def dot(a, b, ca, cb):
    return lax.dot_general(a, b, (((ca,), (cb,)), ((), ())), preferred_element_type=F32)


def gelu_parts(u):
    u2 = u * u
    t = jnp.tanh(u * (KAPPA + (KAPPA * 0.044715) * u2))
    cdf = 0.5 + 0.5 * t
    return u2, t, cdf


def gelu_low(u):
    _, _, cdf = gelu_parts(u)
    return (u * cdf).astype(BF)


def gelu_both(u):
    u2, t, cdf = gelu_parts(u)
    grad = cdf + (0.5 * u) * (1.0 - t * t) * (KAPPA + (3.0 * KAPPA * 0.044715) * u2)
    return (u * cdf).astype(BF), grad


def position():
    me = lax.axis_index("data")
    bits = [(me // (2 << d)) % 2 for d in range(3)]
    cores = me % 2
    partner = [me + (2 << d) * (1 - 2 * bits[d]) for d in range(3)]
    return cores, me + 1 - 2 * cores, bits, partner


class Unit:
    def __init__(self, grad, recv, hold, whole, size, send, take, pos):
        self.grad, self.recv, self.hold, self.whole = grad, recv, hold, whole
        self.size, self.send, self.take = size, send, take
        self.core, self.mate, bits, partner = pos
        self.dims = [[(k + s) % 3 for s in range(3)] for k in range(NC)]
        self.bit = [[bits[d] for d in self.dims[k]] for k in range(NC)]
        self.to = [[partner[d] for d in self.dims[k]] for k in range(NC)]

    def rows(self, start, count):
        return pl.ds(pl.multiple_of(start, 16), count)

    def low(self, k, s):
        at = 0
        for step in range(s):
            at = at + self.bit[k][step] * (self.size >> (step + 1))
        return at

    def halving(self, k, s):
        if s == 0:
            return self.copy(self.grad(k, 1 - self.core, None), self.recv(0, k), self.mate, s, k)
        count = self.size >> s
        away = self.low(k, s - 1) + (1 - self.bit[k][s - 1]) * count
        return self.copy(self.grad(k, self.core, self.rows(away, count)), self.recv(s, k), self.to[k][s - 1], s, k)

    def doubling(self, k, s):
        part = self.rows(self.low(k, s) - self.low(k, 1), self.size >> s)
        return self.copy(self.hold(k, part), self.hold(k, part), self.to[k][s - 1], 7 - s, k)

    def across(self, k, s):
        own, mine, far, both = self.whole
        src, dst, dev = {6: (own, mine, self.mate), 7: (own, far, self.to[k][0]), 8: (far, both, self.mate)}[s]
        return self.copy(src(k), dst(k), dev, s, k)

    def step(self, s, k):
        if s < 4:
            return self.halving(k, s)
        return self.doubling(k, 7 - s) if s < 6 else self.across(k, s)

    def copy(self, src, dst, dev, s, k):
        return pltpu.make_async_remote_copy(
            src_ref=src, dst_ref=dst, send_sem=self.send(s, k), recv_sem=self.take(s, k),
            device_id=(dev,), device_id_type=MESH)

    def start(self, s):
        for k in range(NC):
            self.step(s, k).start()

    def wait(self, s):
        for k in range(NC):
            self.step(s, k).wait()

    def follow(self, s, *nexts):
        for k in range(NC):
            self.step(s, k).wait()
            for n in nexts:
                self.step(n, k).start()

    def reduce(self, s):
        for k in range(NC):
            self.step(s, k).wait()
            count = self.size >> s
            mine = self.grad(k, self.core, self.rows(self.low(k, s), count))
            total = mine[...] + self.recv(s, k)[...]
            if s < 3:
                mine[...] = total
                self.halving(k, s + 1).start()
            else:
                self.hold(k, self.rows(self.low(k, 3) - self.low(k, 1), count))[...] = total
                self.doubling(k, 3).start()


def first_kernel(scale, *refs):
    w_in, w_up, w_down, x_hbm, y_hbm = refs[:5]
    n_out = N_OUT
    out = refs[5:5 + n_out]
    (st1, st2, acts, grads, gin, r0, r1, r2, r3, q0, q1, q2, q3, hold, mates, far, both, hin, min_, fin, bin_,
     xb, yb, state, low, send, take, send_in, take_in, ld1, ld2, ldx, ho, hx) = refs[5 + n_out:]
    pos = position()

    barrier = pltpu.get_barrier_semaphore()
    for dev in [pos[1]] + pos[3]:
        pl.semaphore_signal(barrier, inc=1, device_id=(dev,), device_id_type=MESH)

    def load1(l):
        return pltpu.make_async_copy(w_up.at[l], st1.at[l % 2], ld1.at[l % 2])

    def load2(l):
        return pltpu.make_async_copy(w_down.at[l], st2.at[l % 2], ld2.at[l % 2])

    load_x = pltpu.make_async_copy(x_hbm, xb, ldx.at[0])
    load_y = pltpu.make_async_copy(y_hbm, yb, ldx.at[1])
    load_a = pltpu.make_async_copy(w_in.at[pl.ds(0, 1536)], st2.at[0], ld2.at[0])
    load_b = pltpu.make_async_copy(w_in.at[pl.ds(1536, 768)], st2.at[1, pl.ds(0, 768)], ld2.at[1])
    load_x.start()
    load_a.start()
    load_b.start()
    load1(0).start()
    load1(1).start()
    load_y.start()
    load_x.wait()
    load_a.wait()
    state[...] = dot(xb[:, :1536], st2[0].astype(BF), 1, 0)
    load2(0).start()
    load_b.wait()
    state[...] += dot(xb[:, 1536:], st2[1, :768].astype(BF), 1, 0)
    load2(1).start()

    @pl.loop(0, L)
    def _(l):
        slot = l % 2
        p = state[...].astype(BF)
        acts[l] = p
        load1(l).wait()
        load2(l).wait()

        for j in range(NC):
            cols = slice(j * 512, j * 512 + 512)
            a = gelu_low(dot(p, st1[slot, :, cols].astype(BF), 1, 0))
            state[...] += dot(a, st2[slot, cols, :].astype(BF), 1, 0)

        @pl.when(l + 2 < L)
        def _():
            load1(l + 2).start()
            load2(l + 2).start()

    pl.semaphore_wait(barrier, 4)
    load_y.wait()
    state[...] = (state[...] - yb[...].astype(F32)) * scale

    def job(i):
        par = i % 2

        def recv(s, k):
            return (r0, r1, r2, r3)[s].at[par, k]

        def grad(k, c, rows):
            ref = grads.at[i % 4, k, c]
            return ref if rows is None else ref.at[:, rows, :]

        whole = (lambda k: hold.at[i % 4, k], lambda k: mates.at[i % 3, k], lambda k: far.at[k], lambda k: both.at[k])
        return Unit(grad, recv, lambda k, rows: hold.at[i % 4, k, :, rows, :], whole, 256,
                    lambda s, k: send.at[s, par, k], lambda s, k: take.at[s, par, k], pos)

    def job_in():
        def grad(k, c, rows):
            ref = gin.at[k, c]
            return ref if rows is None else ref.at[rows, :]

        return Unit(grad, lambda s, k: (q0, q1, q2, q3)[s].at[k], lambda k, rows: hin.at[k, rows, :],
                    tuple((lambda k, ref=ref: ref.at[k]) for ref in (hin, min_, fin, bin_)), 384,
                    lambda s, k: send_in.at[s, k], lambda s, k: take_in.at[s, k], pos)

    def put(i, which, begin):
        l = L - 1 - i
        for g, (first, count) in enumerate(GROUPS):
            @pl.when((l >= first) & (l < first + count))
            def _():
                for k in range(NC):
                    c = pltpu.make_async_copy(hold.at[i % 4, k] if which == 0 else mates.at[i % 3, k],
                                              out[(g * 2 + which) * NC + k].at[l - first], ho.at[i % 2, which, k])
                    if begin:
                        c.start()
                    else:
                        c.wait()

    def during(i, lag, step):
        pl.when((i >= lag) & (i < L + lag))(step)

    def middle(i):
        during(i, 2, lambda: job(i - 2).reduce(1))
        pl.when(i == 18)(lambda: job_in().reduce(1))
        during(i, 1, lambda: job(i - 1).reduce(0))
        pl.when(i == 17)(lambda: job_in().reduce(0))

        @functools.partial(during, i, 6)
        def _():
            put(i - 6, 0, False)
            put(i - 6, 1, False)

        during(i, 3, lambda: job(i - 3).reduce(3))
        pl.when(i == 19)(lambda: job_in().reduce(3))

        @functools.partial(during, i, 5)
        def _():
            job(i - 5).follow(5, 6)
            put(i - 5, 0, True)

        pl.when(i == L + 4)(lambda: job(L - 1).start(7))
        during(i, 4, lambda: job(i - 4).follow(4, 5))

    def end(i):
        during(i, 2, lambda: job(i - 2).reduce(2))
        pl.when(i == 18)(lambda: job_in().reduce(2))
        pl.when(i == 19)(lambda: job_in().follow(4, 5))

        @functools.partial(during, i, 5)
        def _():
            job(i - 5).wait(6)
            put(i - 5, 1, True)


    @pl.loop(0, L + 5)
    def _(i):
        @pl.when(i < L)
        def _():
            @pl.when(i >= 2)
            def _():
                load1(L - 1 - i).wait()
                load2(L - 1 - i).wait()

            low[...] = state[...].astype(BF)

        @pl.loop(0, NC)
        def _(k):
            pl.when(k == 0)(lambda: middle(i))
            pl.when(k == 2)(lambda: end(i))

            @pl.when(i < L)
            def _():
                slot = (L - 1 - i) % 2
                p = acts[L - 1 - i]
                cot = low[...]
                add = None
                for half in range(2):
                    at = pl.multiple_of(k * 512 + half * 256, 256)
                    cols = pl.ds(at, 256)
                    w1 = st1[slot, :, cols].astype(BF)
                    w2 = st2[slot, cols, :].astype(BF)
                    a, slope = gelu_both(dot(p, w1, 1, 0))
                    q = (dot(cot, w2, 1, 1) * slope).astype(BF)
                    grads[i % 4, k, half, 1] = dot(a, cot, 0, 0).astype(BF)
                    grads[i % 4, k, half, 0] = dot(q, p, 0, 0).astype(BF)
                    part = dot(q, w1, 1, 1)
                    add = part if add is None else add + part
                state[...] += add
                job(i).halving(k, 0).start()

        @pl.when(i + 2 < L)
        def _():
            load1(L - 3 - i).start()
            load2(L - 3 - i).start()

        @pl.when(i == L)
        def _():
            low[...] = state[...].astype(BF)

            @pl.loop(0, NC)
            def _(k):
                for half in range(2):
                    cols = pl.ds(pl.multiple_of(k * 768 + half * 384, 384), 384)
                    gin[k, half] = dot(xb[:, cols], low[...], 0, 0).astype(BF)
                job_in().halving(k, 0).start()

    last, entry = job(L - 1), job_in()
    entry.follow(5, 7, 6)
    last.follow(7, 8)
    entry.follow(7, 8)
    entry.wait(6)
    last.wait(8)
    entry.wait(8)
    put(L - 1, 0, False)
    put(L - 1, 1, False)
    base = 2 * NC * len(GROUPS)
    leave = []
    for n, ref in enumerate((hin, min_, fin, bin_, far, both)):
        for k in range(NC):
            dst = out[base + n * NC + k]
            leave.append(pltpu.make_async_copy(ref.at[k], dst if n < 4 else dst.at[0], hx.at[n, k]))
    for c in leave:
        c.start()
    for c in leave:
        c.wait()


def first_call(scale, w_in, w_up, w_down, x_rows, y_rows):
    sds = jax.ShapeDtypeStruct
    shapes = [sds((count, 2, 128, D), BF) for _, count in GROUPS for _ in range(2 * NC)]
    shapes += [sds((192, D), BF)] * (4 * NC) + [sds((1, 2, 128, D), BF)] * (2 * NC)
    dma = pltpu.SemaphoreType.DMA
    scratch = [
        pltpu.VMEM((2, D, FF), F32), pltpu.VMEM((2, FF, D), F32),
        pltpu.VMEM((L, ROWS, D), BF),
        pltpu.VMEM((4, NC, 2, 2, 256, D), BF), pltpu.VMEM((NC, 2, 384, D), BF),
        pltpu.VMEM((2, NC, 2, 256, D), BF), pltpu.VMEM((2, NC, 2, 128, D), BF),
        pltpu.VMEM((2, NC, 2, 64, D), BF), pltpu.VMEM((2, NC, 2, 32, D), BF),
        pltpu.VMEM((NC, 384, D), BF), pltpu.VMEM((NC, 192, D), BF),
        pltpu.VMEM((NC, 96, D), BF), pltpu.VMEM((NC, 48, D), BF),
        pltpu.VMEM((4, NC, 2, 128, D), BF), pltpu.VMEM((3, NC, 2, 128, D), BF),
        *[pltpu.VMEM((NC, 2, 128, D), BF)] * 2, *[pltpu.VMEM((NC, 192, D), BF)] * 4,
        pltpu.VMEM((ROWS, E), BF), pltpu.VMEM((ROWS, D), BF),
        pltpu.VMEM((ROWS, D), F32), pltpu.VMEM((ROWS, D), BF),
        *[dma((9, 2, NC))] * 2, *[dma((9, NC))] * 2, *[dma((2,))] * 3, dma((2, 2, NC)), dma((6, NC)),
    ]
    res = pl.pallas_call(
        functools.partial(first_kernel, scale),
        out_shape=shapes,
        in_specs=[ANY] * 5,
        out_specs=[ANY] * len(shapes),
        scratch_shapes=scratch,
        name="train_step",
        cost_estimate=pl.CostEstimate(flops=75 * 10**9, bytes_accessed=200 * 10**6, transcendentals=0),
        compiler_params=pltpu.CompilerParams(collective_id=0, has_side_effects=True, vmem_limit_bytes=67043328),
    )(w_in, w_up, w_down, x_rows, y_rows)
    take3 = lambda n: res[n * NC:(n + 1) * NC]
    n = 2 * len(GROUPS)
    pairs = [(take3(2 * g), take3(2 * g + 1)) for g in range(len(GROUPS))]
    return pairs, [take3(n + r) for r in range(6)]


def place(core, bits, k, r, size):
    c = core if r < 2 else 1 - core
    b = bits[k] if r % 2 == 0 else 1 - bits[k]
    return pl.ds(pl.multiple_of((k * 4 + c * 2 + b) * size, 16), size)


def layers_kernel(eta, first, count, head, *refs):
    n_parts = 4 * NC * (2 if head else 1)
    parts = refs[:4 * NC]
    w1_hbm, m1_hbm, w2_hbm, m2_hbm, h_hbm = refs[n_parts:n_parts + 5]
    rest = refs[n_parts + 5 + (2 if head else 4):]
    if head:
        parts_in = refs[4 * NC:n_parts]
        w_hbm, m_hbm = refs[n_parts + 5:n_parts + 7]
        new_win, new_min = rest[:2]
        rest = rest[2:]
    new_w1, new_m1, new_w2, new_m2, h_out = rest[:5]
    v1, v2, gv, hv, av, gs, ins, outs, hs = rest[5:14]
    core, _, bits, _ = position()

    def load(n, y):
        s = n % 3
        res = [pltpu.make_async_copy(src.at[first + n], dst.at[s, z], ins.at[s, y, z])
               for yy, (a, b, dst) in enumerate(((w1_hbm, m1_hbm, v1), (w2_hbm, m2_hbm, v2)))
               for z, src in enumerate((a, b)) if yy == y]
        for k in range(NC):
            for r in range(4):
                rows = place(core, bits, k, r, 128)
                res.append(pltpu.make_async_copy(parts[k * 4 + r].at[n, y], gv.at[s, y, rows, :], gs.at[s, y, k, r]))
        return res

    def store(n, y):
        s = n % 3
        return [pltpu.make_async_copy(src.at[s, z], dst.at[first + n], outs.at[s, y, z])
                for yy, (src, a, b) in enumerate(((v1, new_w1, new_m1), (v2, new_w2, new_m2)))
                for z, dst in enumerate((a, b)) if yy == y]

    load_h = pltpu.make_async_copy(h_hbm, rest[14] if head else hv, hs.at[0])
    if head:
        xv, wv, mv, gi, gsi, insi, outsi = rest[14:]

        def load_in(k):
            rows = pl.ds(k * 768, 768)
            res = [pltpu.make_async_copy(w_hbm.at[rows], wv.at[rows], insi.at[0, k]),
                   pltpu.make_async_copy(m_hbm.at[rows], mv.at[rows], insi.at[1, k])]
            for r in range(4):
                rows = place(core, bits, k, r, 192)
                res.append(pltpu.make_async_copy(parts_in[k * 4 + r], gi.at[rows], gsi.at[k, r]))
            return res

        def store_in(k):
            rows = pl.ds(k * 768, 768)
            return [pltpu.make_async_copy(wv.at[rows], new_win.at[rows], outsi.at[0, k]),
                    pltpu.make_async_copy(mv.at[rows], new_min.at[rows], outsi.at[1, k])]

        for c in load_in(0) + [load_h] + load_in(1) + load_in(2) + load(0, 0) + load(0, 1):
            c.start()
        for k in range(NC):
            for c in load_in(k) + ([load_h] if k == 0 else []):
                c.wait()
            rows = slice(k * 768, k * 768 + 768)
            m = MOMENTUM * mv[rows, :] + gi[rows, :].astype(F32)
            w = wv[rows, :] - eta * m
            mv[rows, :] = m
            wv[rows, :] = w
            for c in store_in(k):
                c.start()
            part = dot(xv[:, rows], w.astype(BF), 1, 0)
            hv[...] = part if k == 0 else hv[...] + part
    else:
        for c in load(0, 0) + [load_h] + load(0, 1):
            c.start()
        load_h.wait()

    @pl.loop(0, count)
    def _(n):
        s = n % 3

        @pl.when(n >= 2)
        def _():
            for c in store(n - 2, 0) + store(n - 2, 1):
                c.wait()

        @pl.when(n + 1 < count)
        def _():
            for c in load(n + 1, 0) + load(n + 1, 1):
                c.start()

        for c in load(n, 0):
            c.wait()
        p = hv[...].astype(BF)

        @pl.loop(0, NC)
        def _(j):
            for half in range(2):
                cols = pl.ds(pl.multiple_of(j * 512 + half * 256, 256), 256)
                m1 = MOMENTUM * v1[s, 1, :, cols] + gv[s, 0, cols, :].astype(F32).T
                w1 = v1[s, 0, :, cols] - eta * m1
                v1[s, 1, :, cols] = m1
                v1[s, 0, :, cols] = w1
                av[:, cols] = gelu_low(dot(p, w1.astype(BF), 1, 0))

        for c in store(n, 0):
            c.start()
        for c in load(n, 1):
            c.wait()

        @pl.loop(0, NC)
        def _(j):
            cols = pl.ds(pl.multiple_of(j * 512, 512), 512)
            m2 = MOMENTUM * v2[s, 1, cols, :] + gv[s, 1, cols, :].astype(F32)
            w2 = v2[s, 0, cols, :] - eta * m2
            v2[s, 1, cols, :] = m2
            v2[s, 0, cols, :] = w2
            hv[...] += dot(av[:, cols], w2.astype(BF), 1, 0)

        for c in store(n, 1):
            c.start()

    give_h = pltpu.make_async_copy(hv, h_out, hs.at[1])
    give_h.start()
    for n in range(max(0, count - 2), count):
        for c in store(n, 0) + store(n, 1):
            c.wait()
    if head:
        for k in range(NC):
            for c in store_in(k):
                c.wait()
    give_h.wait()


def layers_call(eta, first, count, parts, arrays, h, made, head=None):
    sds = jax.ShapeDtypeStruct
    dma = pltpu.SemaphoreType.DMA
    flat = [p for k in range(NC) for p in parts[k]]
    if head:
        flat += [p for k in range(NC) for p in head[0][k]]
    n = len(flat)
    more = list(head[1:]) if head else list(made)
    shapes = [sds((E, D), F32)] * 2 if head else []
    up, down = sds((L, D, FF), F32), sds((L, FF, D), F32)
    shapes += [up, up, down, down, sds((ROWS, D), F32)]
    scratch = [pltpu.VMEM((3, 2, D, FF), F32), pltpu.VMEM((3, 2, FF, D), F32),
               pltpu.VMEM((3, 2, FF, D), BF), pltpu.VMEM((ROWS, D), F32), pltpu.VMEM((ROWS, FF), BF),
               dma((3, 2, NC, 4)), dma((3, 2, 2)), dma((3, 2, 2)), dma((2,))]
    if head:
        scratch += [pltpu.VMEM((ROWS, E), BF), pltpu.VMEM((E, D), F32), pltpu.VMEM((E, D), F32),
                    pltpu.VMEM((E, D), BF), dma((NC, 4)), dma((2, NC)), dma((2, NC))]
    return pl.pallas_call(
        functools.partial(layers_kernel, eta, first, count, head is not None),
        out_shape=shapes,
        in_specs=[ANY] * (n + 5 + len(more)),
        out_specs=[ANY] * len(shapes),
        input_output_aliases={} if head else {n + 5 + r: r for r in range(4)},
        scratch_shapes=scratch,
        cost_estimate=pl.CostEstimate(flops=count * 6 * 10**9, bytes_accessed=count * 21 * 10**6, transcendentals=0),
        compiler_params=pltpu.CompilerParams(vmem_limit_bytes=67043328),
    )(*flat, *arrays, h, *more)


def solution(mesh):
    group_size = mesh.shape["data"]

    def swap(v, bit):
        return lax.ppermute(v, "data", [(d, d ^ bit) for d in range(group_size)])

    def far_half(own):
        res = []
        for k in range(NC):
            res.append(swap(own[k], 2 << k))
        return res

    def complete(own, mate, other, after):
        other = lax.optimization_barrier((*other, after))[:NC]
        res = []
        for k in range(NC):
            res.append((own[k], other[k], mate[k], swap(other[k], 1)))
        return res

    def device_steps(w_in, w_up, w_down, mom_in, mom_up, mom_down, x_now, y_now, x_next, y_next):
        eta = 4.0 * D / (FF * (L + 1))
        scale = 1.0 / (ROWS * group_size * D)
        pairs, (own, mate, other, both, other0, both0) = first_call(scale, w_in, w_up, w_down, x_now, y_now)
        parts_in = [(own[k], other[k], mate[k], both[k]) for k in range(NC)]
        parts = [[(pairs[0][0][k], other0[k], pairs[0][1][k], both0[k]) for k in range(NC)]]
        others = [far_half(pair[0]) for pair in pairs[1:]]
        arrays = (w_up, mom_up, w_down, mom_down)
        parts.append(complete(*pairs[1], others[0], pairs[0][0][0]))
        for g, (first, count) in enumerate(GROUPS):
            if g in (1, 3):
                parts.append(complete(*pairs[len(parts)], others[len(parts) - 1], h))
            if g == 0:
                new_w_in, new_mom_in, *made, h = layers_call(eta, first, count, parts[0], arrays, x_next, None,
                                                             (parts_in, w_in, mom_in))
            else:
                *made, h = layers_call(eta, first, count, parts[g], arrays, h, made)
        new_w_up, new_mom_up, new_w_down, new_mom_down = made
        loss = jnp.sum(jnp.square(h - y_next.astype(F32)), axis=1) / (2 * D)
        return (new_w_in, new_w_up, new_w_down, new_mom_in, new_mom_up, new_mom_down, loss, h)

    param_spec = P()
    row_spec = P("data", None)
    return jax.shard_map(
        device_steps,
        mesh=mesh,
        in_specs=(param_spec,) * 6 + (row_spec,) * 4,
        out_specs=(param_spec,) * 6 + (P("data"), row_spec),
        check_vma=False,
    )
```

```python
import functools

import jax
import jax.numpy as jnp
from jax import lax
from jax.experimental import pallas as pl
from jax.experimental.pallas import tpu as pltpu
from jax.sharding import PartitionSpec as P


MOMENTUM = 0.9
BF = jnp.bfloat16
F32 = jnp.float32
MESH = pl.DeviceIdType.MESH
ANY = pl.BlockSpec(memory_space=pl.ANY)
VM = pl.BlockSpec(memory_space=pltpu.VMEM)
L, D, FF, E, ROWS = 16, 384, 1536, 2304, 512
NC = 3
GROUPS = ((0, 1), (1, 1), (2, 4), (6, 10))
CALLS = ((0, 0, 1), (1, 1, 1), (2, 2, 3), (2, 5, 1), (3, 6, 10))
N_OUT = NC * (2 * len(GROUPS) + 6)
KAPPA = 0.7978845608028654


def dot(a, b, ca, cb):
    return lax.dot_general(a, b, (((ca,), (cb,)), ((), ())), preferred_element_type=F32)


def gelu_parts(u):
    u2 = u * u
    t = jnp.tanh(u * (KAPPA + (KAPPA * 0.044715) * u2))
    cdf = 0.5 + 0.5 * t
    return u2, t, cdf


def gelu_low(u):
    _, _, cdf = gelu_parts(u)
    return (u * cdf).astype(BF)


def gelu_both(u):
    u2, t, cdf = gelu_parts(u)
    grad = cdf + (0.5 * u) * (1.0 - t * t) * (KAPPA + (3.0 * KAPPA * 0.044715) * u2)
    return (u * cdf).astype(BF), grad


def position():
    me = lax.axis_index("data")
    bits = [(me // (2 << d)) % 2 for d in range(3)]
    cores = me % 2
    partner = [me + (2 << d) * (1 - 2 * bits[d]) for d in range(3)]
    return cores, me + 1 - 2 * cores, bits, partner


class Unit:
    def __init__(self, grad, recv, hold, whole, size, send, take, pos):
        self.grad, self.recv, self.hold, self.whole = grad, recv, hold, whole
        self.size, self.send, self.take = size, send, take
        self.core, self.mate, bits, partner = pos
        self.dims = [[(k + s) % 3 for s in range(3)] for k in range(NC)]
        self.bit = [[bits[d] for d in self.dims[k]] for k in range(NC)]
        self.to = [[partner[d] for d in self.dims[k]] for k in range(NC)]

    def rows(self, start, count):
        return pl.ds(pl.multiple_of(start, 16), count)

    def low(self, k, s):
        at = 0
        for step in range(s):
            at = at + self.bit[k][step] * (self.size >> (step + 1))
        return at

    def halving(self, k, s):
        if s == 0:
            return self.copy(self.grad(k, 1 - self.core, None), self.recv(0, k), self.mate, s, k)
        count = self.size >> s
        away = self.low(k, s - 1) + (1 - self.bit[k][s - 1]) * count
        return self.copy(self.grad(k, self.core, self.rows(away, count)), self.recv(s, k), self.to[k][s - 1], s, k)

    def doubling(self, k, s):
        part = self.rows(self.low(k, s) - self.low(k, 1), self.size >> s)
        return self.copy(self.hold(k, part), self.hold(k, part), self.to[k][s - 1], 7 - s, k)

    def across(self, k, s):
        own, mine, far, both = self.whole
        src, dst, dev = {6: (own, mine, self.mate), 7: (own, far, self.to[k][0]), 8: (far, both, self.mate)}[s]
        return self.copy(src(k), dst(k), dev, s, k)

    def step(self, s, k):
        if s < 4:
            return self.halving(k, s)
        return self.doubling(k, 7 - s) if s < 6 else self.across(k, s)

    def copy(self, src, dst, dev, s, k):
        return pltpu.make_async_remote_copy(
            src_ref=src, dst_ref=dst, send_sem=self.send(s, k), recv_sem=self.take(s, k),
            device_id=(dev,), device_id_type=MESH)

    def start(self, s):
        for k in range(NC):
            self.step(s, k).start()

    def wait(self, s):
        for k in range(NC):
            self.step(s, k).wait()

    def follow(self, s, *nexts):
        for k in range(NC):
            self.step(s, k).wait()
            for n in nexts:
                self.step(n, k).start()

    def reduce(self, s):
        for k in range(NC):
            self.step(s, k).wait()
            count = self.size >> s
            mine = self.grad(k, self.core, self.rows(self.low(k, s), count))
            total = mine[...] + self.recv(s, k)[...]
            if s < 3:
                mine[...] = total
                self.halving(k, s + 1).start()
            else:
                self.hold(k, self.rows(self.low(k, 3) - self.low(k, 1), count))[...] = total
                self.doubling(k, 3).start()


def first_kernel(scale, *refs):
    w_in, w_up, w_down, x_hbm, y_hbm = refs[:5]
    n_out = N_OUT
    out = refs[5:5 + n_out]
    (win, st1, st2, acts, grads, gin, r0, r1, r2, r3, q0, q1, q2, q3, hold, mates, far, both, hin, min_, fin, bin_,
     xb, yb, state, turned, low, send, take, send_in, take_in, ld1, ld2, ldx, ho, hx) = refs[5 + n_out:]
    pos = position()

    barrier = pltpu.get_barrier_semaphore()
    for dev in [pos[1]] + pos[3]:
        pl.semaphore_signal(barrier, inc=1, device_id=(dev,), device_id_type=MESH)

    def load1(l):
        return pltpu.make_async_copy(w_up.at[l], st1.at[l % 2], ld1.at[l % 2])

    def load2(l):
        return pltpu.make_async_copy(w_down.at[l], st2.at[l % 2], ld2.at[l % 2])

    load_x = pltpu.make_async_copy(x_hbm, xb, ldx.at[0])
    load_y = pltpu.make_async_copy(y_hbm, yb, ldx.at[1])
    load_x.start()
    pieces = []
    for k in range(NC):
        rows = pl.ds(k * 768, 768)
        pieces.append(pltpu.make_async_copy(w_in.at[rows], win.at[rows], ldx.at[2 + k]))
        pieces[k].start()
    for l in range(2):
        load1(l).start()
        load2(l).start()
    load_y.start()
    load_x.wait()
    for k in range(NC):
        rows = slice(k * 768, k * 768 + 768)
        pieces[k].wait()
        part = dot(xb[:, rows], win[rows, :].astype(BF), 1, 0)
        state[...] = part if k == 0 else state[...] + part
    turned[...] = state[...].T

    @pl.loop(0, L)
    def _(l):
        slot = l % 2
        p = turned[...].T.astype(BF)
        acts[l] = p
        load1(l).wait()
        load2(l).wait()

        for j in range(NC):
            cols = slice(j * 512, j * 512 + 512)
            a = gelu_low(dot(p, st1[slot, :, cols].astype(BF), 1, 0))
            turned[...] += dot(st2[slot, cols, :].astype(BF), a, 0, 1)

        @pl.when(l + 2 < L)
        def _():
            load1(l + 2).start()
            load2(l + 2).start()

    pl.semaphore_wait(barrier, 4)
    load_y.wait()
    state[...] = (turned[...].T - yb[...].astype(F32)) * scale

    def job(i):
        par = i % 2

        def recv(s, k):
            return (r0, r1, r2, r3)[s].at[par, k]

        def grad(k, c, rows):
            ref = grads.at[i % 4, k, c]
            return ref if rows is None else ref.at[:, rows, :]

        whole = (lambda k: hold.at[i % 4, k], lambda k: mates.at[i % 3, k], lambda k: far.at[k], lambda k: both.at[k])
        return Unit(grad, recv, lambda k, rows: hold.at[i % 4, k, :, rows, :], whole, 256,
                    lambda s, k: send.at[s, par, k], lambda s, k: take.at[s, par, k], pos)

    def job_in():
        def grad(k, c, rows):
            ref = gin.at[k, c]
            return ref if rows is None else ref.at[rows, :]

        return Unit(grad, lambda s, k: (q0, q1, q2, q3)[s].at[k], lambda k, rows: hin.at[k, rows, :],
                    tuple((lambda k, ref=ref: ref.at[k]) for ref in (hin, min_, fin, bin_)), 384,
                    lambda s, k: send_in.at[s, k], lambda s, k: take_in.at[s, k], pos)

    def put(i, which, begin):
        l = L - 1 - i
        for g, (first, count) in enumerate(GROUPS):
            @pl.when((l >= first) & (l < first + count))
            def _():
                for k in range(NC):
                    c = pltpu.make_async_copy(hold.at[i % 4, k] if which == 0 else mates.at[i % 3, k],
                                              out[(g * 2 + which) * NC + k].at[l - first], ho.at[i % 2, which, k])
                    if begin:
                        c.start()
                    else:
                        c.wait()

    def during(i, lag, step):
        pl.when((i >= lag) & (i < L + lag))(step)

    def middle(i):
        during(i, 2, lambda: job(i - 2).reduce(1))
        pl.when(i == 18)(lambda: job_in().reduce(1))
        during(i, 1, lambda: job(i - 1).reduce(0))
        pl.when(i == 17)(lambda: job_in().reduce(0))

        @functools.partial(during, i, 6)
        def _():
            put(i - 6, 0, False)
            put(i - 6, 1, False)

        during(i, 3, lambda: job(i - 3).reduce(3))
        pl.when(i == 19)(lambda: job_in().reduce(3))

        @functools.partial(during, i, 5)
        def _():
            job(i - 5).follow(5, 6)
            put(i - 5, 0, True)

        pl.when(i == L + 4)(lambda: job(L - 1).start(7))
        during(i, 4, lambda: job(i - 4).follow(4, 5))

    def end(i):
        during(i, 2, lambda: job(i - 2).reduce(2))
        pl.when(i == 18)(lambda: job_in().reduce(2))
        pl.when(i == 19)(lambda: job_in().follow(4, 5))

        @functools.partial(during, i, 5)
        def _():
            job(i - 5).wait(6)
            put(i - 5, 1, True)


    @pl.loop(0, L + 5)
    def _(i):
        @pl.when(i < L)
        def _():
            @pl.when(i >= 2)
            def _():
                load1(L - 1 - i).wait()
                load2(L - 1 - i).wait()

            low[...] = state[...].astype(BF)

        @pl.loop(0, NC)
        def _(k):
            pl.when(k == 0)(lambda: middle(i))
            pl.when(k == 2)(lambda: end(i))

            @pl.when(i < L)
            def _():
                slot = (L - 1 - i) % 2
                p = acts[L - 1 - i]
                cot = low[...]
                add = None
                for half in range(2):
                    at = pl.multiple_of(k * 512 + half * 256, 256)
                    cols = pl.ds(at, 256)
                    w1 = st1[slot, :, cols].astype(BF)
                    w2 = st2[slot, cols, :].astype(BF)
                    a, slope = gelu_both(dot(p, w1, 1, 0))
                    q = (dot(cot, w2, 1, 1) * slope).astype(BF)
                    grads[i % 4, k, half, 1] = dot(a, cot, 0, 0).astype(BF)
                    grads[i % 4, k, half, 0] = dot(q, p, 0, 0).astype(BF)
                    part = dot(q, w1, 1, 1)
                    add = part if add is None else add + part
                state[...] += add
                job(i).halving(k, 0).start()

        @pl.when(i + 2 < L)
        def _():
            load1(L - 3 - i).start()
            load2(L - 3 - i).start()

        @pl.when(i == L)
        def _():
            low[...] = state[...].astype(BF)

            @pl.loop(0, NC)
            def _(k):
                for half in range(2):
                    cols = pl.ds(pl.multiple_of(k * 768 + half * 384, 384), 384)
                    gin[k, half] = dot(xb[:, cols], low[...], 0, 0).astype(BF)
                job_in().halving(k, 0).start()

    last, entry = job(L - 1), job_in()
    entry.follow(5, 7, 6)
    last.follow(7, 8)
    entry.follow(7, 8)
    entry.wait(6)
    last.wait(8)
    entry.wait(8)
    put(L - 1, 0, False)
    put(L - 1, 1, False)
    base = 2 * NC * len(GROUPS)
    leave = []
    for n, ref in enumerate((hin, min_, fin, bin_, far, both)):
        for k in range(NC):
            dst = out[base + n * NC + k]
            leave.append(pltpu.make_async_copy(ref.at[k], dst if n < 4 else dst.at[0], hx.at[n, k]))
    for c in leave:
        c.start()
    for c in leave:
        c.wait()


def first_call(scale, w_in, w_up, w_down, x_rows, y_rows):
    sds = jax.ShapeDtypeStruct
    shapes = [sds((count, 2, 128, D), BF) for _, count in GROUPS for _ in range(2 * NC)]
    shapes += [sds((192, D), BF)] * (4 * NC) + [sds((1, 2, 128, D), BF)] * (2 * NC)
    dma = pltpu.SemaphoreType.DMA
    scratch = [
        pltpu.VMEM((E, D), F32), pltpu.VMEM((2, D, FF), F32), pltpu.VMEM((2, FF, D), F32),
        pltpu.VMEM((L, ROWS, D), BF),
        pltpu.VMEM((4, NC, 2, 2, 256, D), BF), pltpu.VMEM((NC, 2, 384, D), BF),
        pltpu.VMEM((2, NC, 2, 256, D), BF), pltpu.VMEM((2, NC, 2, 128, D), BF),
        pltpu.VMEM((2, NC, 2, 64, D), BF), pltpu.VMEM((2, NC, 2, 32, D), BF),
        pltpu.VMEM((NC, 384, D), BF), pltpu.VMEM((NC, 192, D), BF),
        pltpu.VMEM((NC, 96, D), BF), pltpu.VMEM((NC, 48, D), BF),
        pltpu.VMEM((4, NC, 2, 128, D), BF), pltpu.VMEM((3, NC, 2, 128, D), BF),
        *[pltpu.VMEM((NC, 2, 128, D), BF)] * 2, *[pltpu.VMEM((NC, 192, D), BF)] * 4,
        pltpu.VMEM((ROWS, E), BF), pltpu.VMEM((ROWS, D), BF),
        pltpu.VMEM((ROWS, D), F32), pltpu.VMEM((D, ROWS), F32), pltpu.VMEM((ROWS, D), BF),
        *[dma((9, 2, NC))] * 2, *[dma((9, NC))] * 2, *[dma((2,))] * 2, dma((2 + NC,)), dma((2, 2, NC)), dma((6, NC)),
    ]
    res = pl.pallas_call(
        functools.partial(first_kernel, scale),
        out_shape=shapes,
        in_specs=[ANY] * 5,
        out_specs=[ANY] * len(shapes),
        scratch_shapes=scratch,
        name="train_step",
        cost_estimate=pl.CostEstimate(flops=75 * 10**9, bytes_accessed=200 * 10**6, transcendentals=0),
        compiler_params=pltpu.CompilerParams(collective_id=0, has_side_effects=True, vmem_limit_bytes=67043328),
    )(w_in, w_up, w_down, x_rows, y_rows)
    take3 = lambda n: res[n * NC:(n + 1) * NC]
    n = 2 * len(GROUPS)
    pairs = [(take3(2 * g), take3(2 * g + 1)) for g in range(len(GROUPS))]
    return pairs, [take3(n + r) for r in range(6)]


def place(core, bits, k, r, size):
    c = core if r < 2 else 1 - core
    b = bits[k] if r % 2 == 0 else 1 - bits[k]
    return pl.ds(pl.multiple_of((k * 4 + c * 2 + b) * size, 16), size)


def layers_kernel(eta, first, count, skip, head, *refs):
    n_parts = 4 * NC * (2 if head else 1)
    parts = refs[:4 * NC]
    w1_hbm, m1_hbm, w2_hbm, m2_hbm, h_hbm = refs[n_parts:n_parts + 5]
    rest = refs[n_parts + 5 + (2 if head else 4):]
    if head:
        parts_in = refs[4 * NC:n_parts]
        w_hbm, m_hbm = refs[n_parts + 5:n_parts + 7]
        new_win, new_min = rest[:2]
        rest = rest[2:]
    new_w1, new_m1, new_w2, new_m2, h_out = rest[:5]
    v1, v2, gv, hv, av, gs, ins, outs, hs = rest[5:14]
    core, _, bits, _ = position()

    def load(n, y):
        s = n % 3
        res = [pltpu.make_async_copy(src.at[first + n], dst.at[s, z], ins.at[s, y, z])
               for yy, (a, b, dst) in enumerate(((w1_hbm, m1_hbm, v1), (w2_hbm, m2_hbm, v2)))
               for z, src in enumerate((a, b)) if yy == y]
        for k in range(NC):
            for r in range(4):
                rows = place(core, bits, k, r, 128)
                res.append(pltpu.make_async_copy(parts[k * 4 + r].at[skip + n, y], gv.at[s, y, rows, :], gs.at[s, y, k, r]))
        return res

    def store(n, y):
        s = n % 3
        return [pltpu.make_async_copy(src.at[s, z], dst.at[first + n], outs.at[s, y, z])
                for yy, (src, a, b) in enumerate(((v1, new_w1, new_m1), (v2, new_w2, new_m2)))
                for z, dst in enumerate((a, b)) if yy == y]

    load_h = pltpu.make_async_copy(h_hbm, rest[14] if head else hv, hs.at[0])
    if head:
        xv, wv, mv, gi, gsi, insi, outsi = rest[14:]

        def load_in(k):
            rows = pl.ds(k * 768, 768)
            res = [pltpu.make_async_copy(w_hbm.at[rows], wv.at[rows], insi.at[0, k]),
                   pltpu.make_async_copy(m_hbm.at[rows], mv.at[rows], insi.at[1, k])]
            for r in range(4):
                rows = place(core, bits, k, r, 192)
                res.append(pltpu.make_async_copy(parts_in[k * 4 + r], gi.at[rows], gsi.at[k, r]))
            return res

        def store_in(k):
            rows = pl.ds(k * 768, 768)
            return [pltpu.make_async_copy(wv.at[rows], new_win.at[rows], outsi.at[0, k]),
                    pltpu.make_async_copy(mv.at[rows], new_min.at[rows], outsi.at[1, k])]

        for c in load_in(0) + [load_h] + load_in(1) + load_in(2) + load(0, 0) + load(0, 1):
            c.start()
        for k in range(NC):
            for c in load_in(k) + ([load_h] if k == 0 else []):
                c.wait()
            rows = slice(k * 768, k * 768 + 768)
            m = MOMENTUM * mv[rows, :] + gi[rows, :].astype(F32)
            w = wv[rows, :] - eta * m
            mv[rows, :] = m
            wv[rows, :] = w
            for c in store_in(k):
                c.start()
            part = dot(xv[:, rows], w.astype(BF), 1, 0)
            hv[...] = part if k == 0 else hv[...] + part
    else:
        for c in load(0, 0) + [load_h] + load(0, 1):
            c.start()
        load_h.wait()

    @pl.loop(0, count)
    def _(n):
        s = n % 3

        @pl.when(n >= 2)
        def _():
            for c in store(n - 2, 0) + store(n - 2, 1):
                c.wait()

        @pl.when(n + 1 < count)
        def _():
            for c in load(n + 1, 0) + load(n + 1, 1):
                c.start()

        for c in load(n, 0):
            c.wait()
        p = hv[...].astype(BF)

        @pl.loop(0, NC)
        def _(j):
            for half in range(2):
                cols = pl.ds(pl.multiple_of(j * 512 + half * 256, 256), 256)
                m1 = MOMENTUM * v1[s, 1, :, cols] + gv[s, 0, cols, :].astype(F32).T
                w1 = v1[s, 0, :, cols] - eta * m1
                v1[s, 1, :, cols] = m1
                v1[s, 0, :, cols] = w1
                av[:, cols] = gelu_low(dot(p, w1.astype(BF), 1, 0))

        for c in store(n, 0):
            c.start()
        for c in load(n, 1):
            c.wait()

        @pl.loop(0, NC)
        def _(j):
            cols = pl.ds(pl.multiple_of(j * 512, 512), 512)
            m2 = MOMENTUM * v2[s, 1, cols, :] + gv[s, 1, cols, :].astype(F32)
            w2 = v2[s, 0, cols, :] - eta * m2
            v2[s, 1, cols, :] = m2
            v2[s, 0, cols, :] = w2
            hv[...] += dot(av[:, cols], w2.astype(BF), 1, 0)

        for c in store(n, 1):
            c.start()

    give_h = pltpu.make_async_copy(hv, h_out, hs.at[1])
    give_h.start()
    for n in range(max(0, count - 2), count):
        for c in store(n, 0) + store(n, 1):
            c.wait()
    if head:
        for k in range(NC):
            for c in store_in(k):
                c.wait()
    give_h.wait()


def layers_call(eta, first, count, skip, parts, arrays, h, made, head=None):
    sds = jax.ShapeDtypeStruct
    dma = pltpu.SemaphoreType.DMA
    flat = [p for k in range(NC) for p in parts[k]]
    if head:
        flat += [p for k in range(NC) for p in head[0][k]]
    n = len(flat)
    more = list(head[1:]) if head else list(made)
    shapes = [sds((E, D), F32)] * 2 if head else []
    up, down = sds((L, D, FF), F32), sds((L, FF, D), F32)
    shapes += [up, up, down, down, sds((ROWS, D), F32)]
    scratch = [pltpu.VMEM((3, 2, D, FF), F32), pltpu.VMEM((3, 2, FF, D), F32),
               pltpu.VMEM((3, 2, FF, D), BF), pltpu.VMEM((ROWS, D), F32), pltpu.VMEM((ROWS, FF), BF),
               dma((3, 2, NC, 4)), dma((3, 2, 2)), dma((3, 2, 2)), dma((2,))]
    if head:
        scratch += [pltpu.VMEM((ROWS, E), BF), pltpu.VMEM((E, D), F32), pltpu.VMEM((E, D), F32),
                    pltpu.VMEM((E, D), BF), dma((NC, 4)), dma((2, NC)), dma((2, NC))]
    return pl.pallas_call(
        functools.partial(layers_kernel, eta, first, count, skip, head is not None),
        out_shape=shapes,
        in_specs=[ANY] * (n + 5 + len(more)),
        out_specs=[ANY] * len(shapes),
        input_output_aliases={} if head else {n + 5 + r: r for r in range(4)},
        scratch_shapes=scratch,
        cost_estimate=pl.CostEstimate(flops=count * 6 * 10**9, bytes_accessed=count * 21 * 10**6, transcendentals=0),
        compiler_params=pltpu.CompilerParams(vmem_limit_bytes=67043328),
    )(*flat, *arrays, h, *more)


def solution(mesh):
    group_size = mesh.shape["data"]

    def swap(v, bit):
        return lax.ppermute(v, "data", [(d, d ^ bit) for d in range(group_size)])

    def far_half(own):
        res = []
        for k in range(NC):
            res.append(swap(own[k], 2 << k))
        return res

    def complete(own, mate, other, after):
        other = lax.optimization_barrier((*other, after))[:NC]
        res = []
        for k in range(NC):
            res.append((own[k], other[k], mate[k], swap(other[k], 1)))
        return res

    def device_steps(w_in, w_up, w_down, mom_in, mom_up, mom_down, x_now, y_now, x_next, y_next):
        eta = 4.0 * D / (FF * (L + 1))
        scale = 1.0 / (ROWS * group_size * D)
        pairs, (own, mate, other, both, other0, both0) = first_call(scale, w_in, w_up, w_down, x_now, y_now)
        parts_in = [(own[k], other[k], mate[k], both[k]) for k in range(NC)]
        parts = [[(pairs[0][0][k], other0[k], pairs[0][1][k], both0[k]) for k in range(NC)]]
        others = [far_half(pair[0]) for pair in pairs[1:]]
        arrays = (w_up, mom_up, w_down, mom_down)
        parts.append(complete(*pairs[1], others[0], pairs[0][0][0]))
        for c, (g, first, count) in enumerate(CALLS):
            if c in (1, 3):
                parts.append(complete(*pairs[len(parts)], others[len(parts) - 1], h))
            skip = first - GROUPS[g][0]
            if c == 0:
                new_w_in, new_mom_in, *made, h = layers_call(eta, first, count, skip, parts[g], arrays, x_next,
                                                             None, (parts_in, w_in, mom_in))
            else:
                *made, h = layers_call(eta, first, count, skip, parts[g], arrays, h, made)
        new_w_up, new_mom_up, new_w_down, new_mom_down = made
        loss = jnp.sum(jnp.square(h - y_next.astype(F32)), axis=1) / (2 * D)
        return (new_w_in, new_w_up, new_w_down, new_mom_in, new_mom_up, new_mom_down, loss, h)

    param_spec = P()
    row_spec = P("data", None)
    return jax.shard_map(
        device_steps,
        mesh=mesh,
        in_specs=(param_spec,) * 6 + (row_spec,) * 4,
        out_specs=(param_spec,) * 6 + (P("data"), row_spec),
        check_vma=False,
    )
```

```python
import functools

import jax
import jax.numpy as jnp
from jax import lax
from jax.experimental import pallas as pl
from jax.experimental.pallas import tpu as pltpu
from jax.sharding import PartitionSpec as P


MOMENTUM = 0.9
BF = jnp.bfloat16
F32 = jnp.float32
MESH = pl.DeviceIdType.MESH
ANY = pl.BlockSpec(memory_space=pl.ANY)
VM = pl.BlockSpec(memory_space=pltpu.VMEM)
L, D, FF, E, ROWS = 16, 384, 1536, 2304, 512
NC = 3
GROUPS = ((0, 1), (1, 2), (3, 4), (7, 9))
CALLS = ((0, 0, 1), (1, 1, 2), (2, 3, 2), (2, 5, 2), (3, 7, 9))
N_OUT = NC * (2 * len(GROUPS) + 6)
KAPPA = 0.7978845608028654


def dot(a, b, ca, cb):
    return lax.dot_general(a, b, (((ca,), (cb,)), ((), ())), preferred_element_type=F32)


def gelu_parts(u):
    u2 = u * u
    t = jnp.tanh(u * (KAPPA + (KAPPA * 0.044715) * u2))
    cdf = 0.5 + 0.5 * t
    return u2, t, cdf


def gelu_low(u):
    _, _, cdf = gelu_parts(u)
    return (u * cdf).astype(BF)


def gelu_both(u):
    u2, t, cdf = gelu_parts(u)
    grad = cdf + (0.5 * u) * (1.0 - t * t) * (KAPPA + (3.0 * KAPPA * 0.044715) * u2)
    return (u * cdf).astype(BF), grad


def position():
    me = lax.axis_index("data")
    bits = [(me // (2 << d)) % 2 for d in range(3)]
    cores = me % 2
    partner = [me + (2 << d) * (1 - 2 * bits[d]) for d in range(3)]
    return cores, me + 1 - 2 * cores, bits, partner


class Unit:
    def __init__(self, grad, recv, hold, whole, size, send, take, pos):
        self.grad, self.recv, self.hold, self.whole = grad, recv, hold, whole
        self.size, self.send, self.take = size, send, take
        self.core, self.mate, bits, partner = pos
        self.dims = [[(k + s) % 3 for s in range(3)] for k in range(NC)]
        self.bit = [[bits[d] for d in self.dims[k]] for k in range(NC)]
        self.to = [[partner[d] for d in self.dims[k]] for k in range(NC)]

    def rows(self, start, count):
        return pl.ds(pl.multiple_of(start, 16), count)

    def low(self, k, s):
        at = 0
        for step in range(s):
            at = at + self.bit[k][step] * (self.size >> (step + 1))
        return at

    def halving(self, k, s):
        if s == 0:
            return self.copy(self.grad(k, 1 - self.core, None), self.recv(0, k), self.mate, s, k)
        count = self.size >> s
        away = self.low(k, s - 1) + (1 - self.bit[k][s - 1]) * count
        return self.copy(self.grad(k, self.core, self.rows(away, count)), self.recv(s, k), self.to[k][s - 1], s, k)

    def doubling(self, k, s):
        part = self.rows(self.low(k, s) - self.low(k, 1), self.size >> s)
        return self.copy(self.hold(k, part), self.hold(k, part), self.to[k][s - 1], 7 - s, k)

    def across(self, k, s):
        own, mine, far, both = self.whole
        src, dst, dev = {6: (own, mine, self.mate), 7: (own, far, self.to[k][0]), 8: (far, both, self.mate)}[s]
        return self.copy(src(k), dst(k), dev, s, k)

    def step(self, s, k):
        if s < 4:
            return self.halving(k, s)
        return self.doubling(k, 7 - s) if s < 6 else self.across(k, s)

    def copy(self, src, dst, dev, s, k):
        return pltpu.make_async_remote_copy(
            src_ref=src, dst_ref=dst, send_sem=self.send(s, k), recv_sem=self.take(s, k),
            device_id=(dev,), device_id_type=MESH)

    def start(self, s):
        for k in range(NC):
            self.step(s, k).start()

    def wait(self, s):
        for k in range(NC):
            self.step(s, k).wait()

    def follow(self, s, *nexts):
        for k in range(NC):
            self.step(s, k).wait()
            for n in nexts:
                self.step(n, k).start()

    def reduce(self, s):
        for k in range(NC):
            self.step(s, k).wait()
            count = self.size >> s
            mine = self.grad(k, self.core, self.rows(self.low(k, s), count))
            total = mine[...] + self.recv(s, k)[...]
            if s < 3:
                mine[...] = total
                self.halving(k, s + 1).start()
            else:
                self.hold(k, self.rows(self.low(k, 3) - self.low(k, 1), count))[...] = total
                self.doubling(k, 3).start()


def first_kernel(scale, *refs):
    w_in, w_up, w_down, x_hbm, y_hbm = refs[:5]
    n_out = N_OUT
    out = refs[5:5 + n_out]
    (win, st1, st2, acts, grads, gin, r0, r1, r2, r3, q0, q1, q2, q3, hold, mates, far, both, hin, min_, fin, bin_,
     xb, yb, state, low, send, take, send_in, take_in, ld1, ld2, ldx, ho, hx) = refs[5 + n_out:]
    pos = position()

    barrier = pltpu.get_barrier_semaphore()
    for dev in [pos[1]] + pos[3]:
        pl.semaphore_signal(barrier, inc=1, device_id=(dev,), device_id_type=MESH)

    def load1(l):
        return pltpu.make_async_copy(w_up.at[l], st1.at[l % 2], ld1.at[l % 2])

    def load2(l):
        return pltpu.make_async_copy(w_down.at[l], st2.at[l % 2], ld2.at[l % 2])

    load_x = pltpu.make_async_copy(x_hbm, xb, ldx.at[0])
    load_y = pltpu.make_async_copy(y_hbm, yb, ldx.at[1])
    load_x.start()
    pieces = []
    for k in range(NC):
        rows = pl.ds(k * 768, 768)
        pieces.append(pltpu.make_async_copy(w_in.at[rows], win.at[rows], ldx.at[2 + k]))
        pieces[k].start()
    for l in range(2):
        load1(l).start()
        load2(l).start()
    load_y.start()
    load_x.wait()
    for k in range(NC):
        rows = slice(k * 768, k * 768 + 768)
        pieces[k].wait()
        part = dot(xb[:, rows], win[rows, :].astype(BF), 1, 0)
        state[...] = part if k == 0 else state[...] + part

    @pl.loop(0, L)
    def _(l):
        slot = l % 2
        p = state[...].astype(BF)
        acts[l] = p
        load1(l).wait()
        load2(l).wait()

        for j in range(NC):
            cols = slice(j * 512, j * 512 + 512)
            a = gelu_low(dot(p, st1[slot, :, cols].astype(BF), 1, 0))
            state[...] += dot(a, st2[slot, cols, :].astype(BF), 1, 0)

        @pl.when(l + 2 < L)
        def _():
            load1(l + 2).start()
            load2(l + 2).start()

    pl.semaphore_wait(barrier, 4)
    load_y.wait()
    state[...] = (state[...] - yb[...].astype(F32)) * scale

    def job(i):
        par = i % 2

        def recv(s, k):
            return (r0, r1, r2, r3)[s].at[par, k]

        def grad(k, c, rows):
            ref = grads.at[i % 4, k, c]
            return ref if rows is None else ref.at[:, rows, :]

        whole = (lambda k: hold.at[i % 4, k], lambda k: mates.at[i % 3, k], lambda k: far.at[k], lambda k: both.at[k])
        return Unit(grad, recv, lambda k, rows: hold.at[i % 4, k, :, rows, :], whole, 256,
                    lambda s, k: send.at[s, par, k], lambda s, k: take.at[s, par, k], pos)

    def job_in():
        def grad(k, c, rows):
            ref = gin.at[k, c]
            return ref if rows is None else ref.at[rows, :]

        return Unit(grad, lambda s, k: (q0, q1, q2, q3)[s].at[k], lambda k, rows: hin.at[k, rows, :],
                    tuple((lambda k, ref=ref: ref.at[k]) for ref in (hin, min_, fin, bin_)), 384,
                    lambda s, k: send_in.at[s, k], lambda s, k: take_in.at[s, k], pos)

    def put(i, which, begin):
        l = L - 1 - i
        for g, (first, count) in enumerate(GROUPS):
            @pl.when((l >= first) & (l < first + count))
            def _():
                for k in range(NC):
                    c = pltpu.make_async_copy(hold.at[i % 4, k] if which == 0 else mates.at[i % 3, k],
                                              out[(g * 2 + which) * NC + k].at[l - first], ho.at[i % 2, which, k])
                    if begin:
                        c.start()
                    else:
                        c.wait()

    def during(i, lag, step):
        pl.when((i >= lag) & (i < L + lag))(step)

    def middle(i):
        pl.when(i == L + 4)(lambda: job_in().follow(5, 7, 6))
        pl.when(i == 17)(lambda: job_in().reduce(0))
        during(i, 2, lambda: job(i - 2).reduce(1))
        pl.when(i == 18)(lambda: job_in().reduce(1))
        during(i, 1, lambda: job(i - 1).reduce(0))

        @functools.partial(during, i, 6)
        def _():
            put(i - 6, 0, False)
            put(i - 6, 1, False)

        during(i, 3, lambda: job(i - 3).reduce(3))
        pl.when(i == 19)(lambda: job_in().reduce(3))

        @functools.partial(during, i, 5)
        def _():
            job(i - 5).follow(5, 6)
            put(i - 5, 0, True)

        pl.when(i == L + 4)(lambda: job(L - 1).start(7))
        during(i, 4, lambda: job(i - 4).follow(4, 5))

    def end(i):
        during(i, 2, lambda: job(i - 2).reduce(2))
        pl.when(i == 18)(lambda: job_in().reduce(2))
        pl.when(i == 19)(lambda: job_in().follow(4, 5))

        @functools.partial(during, i, 5)
        def _():
            job(i - 5).wait(6)
            put(i - 5, 1, True)


    @pl.loop(0, L + 5)
    def _(i):
        @pl.when(i < L)
        def _():
            @pl.when(i >= 2)
            def _():
                load1(L - 1 - i).wait()
                load2(L - 1 - i).wait()

            low[...] = state[...].astype(BF)

        @pl.loop(0, NC)
        def _(k):
            pl.when(k == 0)(lambda: middle(i))
            pl.when(k == 2)(lambda: end(i))

            @pl.when(i < L)
            def _():
                slot = (L - 1 - i) % 2
                p = acts[L - 1 - i]
                cot = low[...]
                add = None
                for half in range(2):
                    at = pl.multiple_of(k * 512 + half * 256, 256)
                    cols = pl.ds(at, 256)
                    w1 = st1[slot, :, cols].astype(BF)
                    w2 = st2[slot, cols, :].astype(BF)
                    a, slope = gelu_both(dot(p, w1, 1, 0))
                    q = (dot(cot, w2, 1, 1) * slope).astype(BF)
                    grads[i % 4, k, half, 1] = dot(a, cot, 0, 0).astype(BF)
                    grads[i % 4, k, half, 0] = dot(q, p, 0, 0).astype(BF)
                    part = dot(q, w1, 1, 1)
                    add = part if add is None else add + part
                state[...] += add
                job(i).halving(k, 0).start()

        @pl.when(i + 2 < L)
        def _():
            load1(L - 3 - i).start()
            load2(L - 3 - i).start()

        @pl.when(i == L)
        def _():
            low[...] = state[...].astype(BF)

            @pl.loop(0, NC)
            def _(k):
                for half in range(2):
                    cols = pl.ds(pl.multiple_of(k * 768 + half * 384, 384), 384)
                    gin[k, half] = dot(xb[:, cols], low[...], 0, 0).astype(BF)
                job_in().halving(k, 0).start()

    last, entry = job(L - 1), job_in()
    entry.follow(7, 8)
    last.follow(7, 8)
    entry.wait(6)
    last.wait(8)
    entry.wait(8)
    put(L - 1, 0, False)
    put(L - 1, 1, False)
    base = 2 * NC * len(GROUPS)
    leave = []
    for n, ref in enumerate((hin, min_, fin, bin_, far, both)):
        for k in range(NC):
            dst = out[base + n * NC + k]
            leave.append(pltpu.make_async_copy(ref.at[k], dst if n < 4 else dst.at[0], hx.at[n, k]))
    for c in leave:
        c.start()
    for c in leave:
        c.wait()


def first_call(scale, w_in, w_up, w_down, x_rows, y_rows):
    sds = jax.ShapeDtypeStruct
    shapes = [sds((count, 2, 128, D), BF) for _, count in GROUPS for _ in range(2 * NC)]
    shapes += [sds((192, D), BF)] * (4 * NC) + [sds((1, 2, 128, D), BF)] * (2 * NC)
    dma = pltpu.SemaphoreType.DMA
    scratch = [
        pltpu.VMEM((E, D), F32), pltpu.VMEM((2, D, FF), F32), pltpu.VMEM((2, FF, D), F32),
        pltpu.VMEM((L, ROWS, D), BF),
        pltpu.VMEM((4, NC, 2, 2, 256, D), BF), pltpu.VMEM((NC, 2, 384, D), BF),
        pltpu.VMEM((2, NC, 2, 256, D), BF), pltpu.VMEM((2, NC, 2, 128, D), BF),
        pltpu.VMEM((2, NC, 2, 64, D), BF), pltpu.VMEM((2, NC, 2, 32, D), BF),
        pltpu.VMEM((NC, 384, D), BF), pltpu.VMEM((NC, 192, D), BF),
        pltpu.VMEM((NC, 96, D), BF), pltpu.VMEM((NC, 48, D), BF),
        pltpu.VMEM((4, NC, 2, 128, D), BF), pltpu.VMEM((3, NC, 2, 128, D), BF),
        *[pltpu.VMEM((NC, 2, 128, D), BF)] * 2, *[pltpu.VMEM((NC, 192, D), BF)] * 4,
        pltpu.VMEM((ROWS, E), BF), pltpu.VMEM((ROWS, D), BF),
        pltpu.VMEM((ROWS, D), F32), pltpu.VMEM((ROWS, D), BF),
        *[dma((9, 2, NC))] * 2, *[dma((9, NC))] * 2, *[dma((2,))] * 2, dma((2 + NC,)), dma((2, 2, NC)), dma((6, NC)),
    ]
    res = pl.pallas_call(
        functools.partial(first_kernel, scale),
        out_shape=shapes,
        in_specs=[ANY] * 5,
        out_specs=[ANY] * len(shapes),
        scratch_shapes=scratch,
        name="train_step",
        cost_estimate=pl.CostEstimate(flops=75 * 10**9, bytes_accessed=200 * 10**6, transcendentals=0),
        compiler_params=pltpu.CompilerParams(collective_id=0, has_side_effects=True, vmem_limit_bytes=67043328),
    )(w_in, w_up, w_down, x_rows, y_rows)
    take3 = lambda n: res[n * NC:(n + 1) * NC]
    n = 2 * len(GROUPS)
    pairs = [(take3(2 * g), take3(2 * g + 1)) for g in range(len(GROUPS))]
    return pairs, [take3(n + r) for r in range(6)]


def place(core, bits, k, r, size):
    c = core if r < 2 else 1 - core
    b = bits[k] if r % 2 == 0 else 1 - bits[k]
    return pl.ds(pl.multiple_of((k * 4 + c * 2 + b) * size, 16), size)


def layers_kernel(eta, first, count, skip, head, *refs):
    n_parts = 4 * NC * (2 if head else 1)
    parts = refs[:4 * NC]
    w1_hbm, m1_hbm, w2_hbm, m2_hbm, h_hbm = refs[n_parts:n_parts + 5]
    rest = refs[n_parts + 5 + (2 if head else 4):]
    if head:
        parts_in = refs[4 * NC:n_parts]
        w_hbm, m_hbm = refs[n_parts + 5:n_parts + 7]
        new_win, new_min = rest[:2]
        rest = rest[2:]
    new_w1, new_m1, new_w2, new_m2, h_out = rest[:5]
    v1, v2, gv, hv, av, gs, ins, outs, hs = rest[5:14]
    core, _, bits, _ = position()

    def load(n, y):
        s = n % 3
        res = [pltpu.make_async_copy(src.at[first + n], dst.at[s, z], ins.at[s, y, z])
               for yy, (a, b, dst) in enumerate(((w1_hbm, m1_hbm, v1), (w2_hbm, m2_hbm, v2)))
               for z, src in enumerate((a, b)) if yy == y]
        for k in range(NC):
            for r in range(4):
                rows = place(core, bits, k, r, 128)
                res.append(pltpu.make_async_copy(parts[k * 4 + r].at[skip + n, y], gv.at[s, y, rows, :], gs.at[s, y, k, r]))
        return res

    def store(n, y):
        s = n % 3
        return [pltpu.make_async_copy(src.at[s, z], dst.at[first + n], outs.at[s, y, z])
                for yy, (src, a, b) in enumerate(((v1, new_w1, new_m1), (v2, new_w2, new_m2)))
                for z, dst in enumerate((a, b)) if yy == y]

    load_h = pltpu.make_async_copy(h_hbm, rest[14] if head else hv, hs.at[0])
    if head:
        xv, wv, mv, gi, gsi, insi, outsi = rest[14:]

        def load_in(k):
            rows = pl.ds(k * 768, 768)
            res = [pltpu.make_async_copy(w_hbm.at[rows], wv.at[rows], insi.at[0, k]),
                   pltpu.make_async_copy(m_hbm.at[rows], mv.at[rows], insi.at[1, k])]
            for r in range(4):
                rows = place(core, bits, k, r, 192)
                res.append(pltpu.make_async_copy(parts_in[k * 4 + r], gi.at[rows], gsi.at[k, r]))
            return res

        def store_in(k):
            rows = pl.ds(k * 768, 768)
            return [pltpu.make_async_copy(wv.at[rows], new_win.at[rows], outsi.at[0, k]),
                    pltpu.make_async_copy(mv.at[rows], new_min.at[rows], outsi.at[1, k])]

        for c in load_in(0) + [load_h] + load_in(1) + load_in(2) + load(0, 0) + load(0, 1):
            c.start()
        for k in range(NC):
            for c in load_in(k) + ([load_h] if k == 0 else []):
                c.wait()
            rows = slice(k * 768, k * 768 + 768)
            m = MOMENTUM * mv[rows, :] + gi[rows, :].astype(F32)
            w = wv[rows, :] - eta * m
            mv[rows, :] = m
            wv[rows, :] = w
            for c in store_in(k):
                c.start()
            part = dot(xv[:, rows], w.astype(BF), 1, 0)
            hv[...] = part if k == 0 else hv[...] + part
    else:
        for c in load(0, 0) + [load_h] + load(0, 1):
            c.start()
        load_h.wait()

    @pl.loop(0, count)
    def _(n):
        s = n % 3

        @pl.when(n >= 2)
        def _():
            for c in store(n - 2, 0) + store(n - 2, 1):
                c.wait()

        @pl.when(n + 1 < count)
        def _():
            for c in load(n + 1, 0) + load(n + 1, 1):
                c.start()

        for c in load(n, 0):
            c.wait()
        p = hv[...].astype(BF)

        @pl.loop(0, NC)
        def _(j):
            for half in range(2):
                cols = pl.ds(pl.multiple_of(j * 512 + half * 256, 256), 256)
                m1 = MOMENTUM * v1[s, 1, :, cols] + gv[s, 0, cols, :].astype(F32).T
                w1 = v1[s, 0, :, cols] - eta * m1
                v1[s, 1, :, cols] = m1
                v1[s, 0, :, cols] = w1
                av[:, cols] = gelu_low(dot(p, w1.astype(BF), 1, 0))

        for c in store(n, 0):
            c.start()
        for c in load(n, 1):
            c.wait()

        @pl.loop(0, NC)
        def _(j):
            cols = pl.ds(pl.multiple_of(j * 512, 512), 512)
            m2 = MOMENTUM * v2[s, 1, cols, :] + gv[s, 1, cols, :].astype(F32)
            w2 = v2[s, 0, cols, :] - eta * m2
            v2[s, 1, cols, :] = m2
            v2[s, 0, cols, :] = w2
            hv[...] += dot(av[:, cols], w2.astype(BF), 1, 0)

        for c in store(n, 1):
            c.start()

    give_h = pltpu.make_async_copy(hv, h_out, hs.at[1])
    give_h.start()
    for n in range(max(0, count - 2), count):
        for c in store(n, 0) + store(n, 1):
            c.wait()
    if head:
        for k in range(NC):
            for c in store_in(k):
                c.wait()
    give_h.wait()


def layers_call(eta, first, count, skip, parts, arrays, h, made, head=None):
    sds = jax.ShapeDtypeStruct
    dma = pltpu.SemaphoreType.DMA
    flat = [p for k in range(NC) for p in parts[k]]
    if head:
        flat += [p for k in range(NC) for p in head[0][k]]
    n = len(flat)
    more = list(head[1:]) if head else list(made)
    shapes = [sds((E, D), F32)] * 2 if head else []
    up, down = sds((L, D, FF), F32), sds((L, FF, D), F32)
    shapes += [up, up, down, down, sds((ROWS, D), F32)]
    scratch = [pltpu.VMEM((3, 2, D, FF), F32), pltpu.VMEM((3, 2, FF, D), F32),
               pltpu.VMEM((3, 2, FF, D), BF), pltpu.VMEM((ROWS, D), F32), pltpu.VMEM((ROWS, FF), BF),
               dma((3, 2, NC, 4)), dma((3, 2, 2)), dma((3, 2, 2)), dma((2,))]
    if head:
        scratch += [pltpu.VMEM((ROWS, E), BF), pltpu.VMEM((E, D), F32), pltpu.VMEM((E, D), F32),
                    pltpu.VMEM((E, D), BF), dma((NC, 4)), dma((2, NC)), dma((2, NC))]
    return pl.pallas_call(
        functools.partial(layers_kernel, eta, first, count, skip, head is not None),
        out_shape=shapes,
        in_specs=[ANY] * (n + 5 + len(more)),
        out_specs=[ANY] * len(shapes),
        input_output_aliases={} if head else {n + 5 + r: r for r in range(4)},
        scratch_shapes=scratch,
        cost_estimate=pl.CostEstimate(flops=count * 6 * 10**9, bytes_accessed=count * 21 * 10**6, transcendentals=0),
        compiler_params=pltpu.CompilerParams(vmem_limit_bytes=67043328),
    )(*flat, *arrays, h, *more)


def solution(mesh):
    group_size = mesh.shape["data"]

    def swap(v, bit):
        return lax.ppermute(v, "data", [(d, d ^ bit) for d in range(group_size)])

    def far_half(own):
        res = []
        for k in range(NC):
            res.append(swap(own[k], 2 << k))
        return res

    def complete(own, mate, other, after):
        other = lax.optimization_barrier((*other, after))[:NC]
        res = []
        for k in range(NC):
            res.append((own[k], other[k], mate[k], swap(other[k], 1)))
        return res

    def device_steps(w_in, w_up, w_down, mom_in, mom_up, mom_down, x_now, y_now, x_next, y_next):
        eta = 4.0 * D / (FF * (L + 1))
        scale = 1.0 / (ROWS * group_size * D)
        pairs, (own, mate, other, both, other0, both0) = first_call(scale, w_in, w_up, w_down, x_now, y_now)
        parts_in = [(own[k], other[k], mate[k], both[k]) for k in range(NC)]
        parts = [[(pairs[0][0][k], other0[k], pairs[0][1][k], both0[k]) for k in range(NC)]]
        others = [far_half(pair[0]) for pair in pairs[1:]]
        arrays = (w_up, mom_up, w_down, mom_down)
        parts.append(complete(*pairs[1], others[0], pairs[0][0][0]))
        for c, (g, first, count) in enumerate(CALLS):
            if c in (1, 3):
                parts.append(complete(*pairs[len(parts)], others[len(parts) - 1], h))
            skip = first - GROUPS[g][0]
            if c == 0:
                new_w_in, new_mom_in, *made, h = layers_call(eta, first, count, skip, parts[g], arrays, x_next,
                                                             None, (parts_in, w_in, mom_in))
            else:
                *made, h = layers_call(eta, first, count, skip, parts[g], arrays, h, made)
        new_w_up, new_mom_up, new_w_down, new_mom_down = made
        loss = jnp.sum(jnp.square(h - y_next.astype(F32)), axis=1) / (2 * D)
        return (new_w_in, new_w_up, new_w_down, new_mom_in, new_mom_up, new_mom_down, loss, h)

    param_spec = P()
    row_spec = P("data", None)
    return jax.shard_map(
        device_steps,
        mesh=mesh,
        in_specs=(param_spec,) * 6 + (row_spec,) * 4,
        out_specs=(param_spec,) * 6 + (P("data"), row_spec),
        check_vma=False,
    )
```
